256 devices in a mesh: blk: 64 (over x, z, core), head: 4 (over y).
Axes of the slice: x: 4, y: 4, z: 8, core: 2. Of those that a mesh axis runs over, the one named last changes fastest.
Arguments:
- ctx_q: bfloat16 [65536, 4096], P('blk', 'head'), may hold values from -120 to 120, as said below
- ctx_k: bfloat16 [65536, 1024], P('blk', 'head'), may hold values from -6 to 6
- ctx_v: bfloat16 [65536, 1024], P('blk', 'head'), may hold values from -6 to 6
- query_q: bfloat16 [64, 256, 4096], P('blk', None, 'head'), may hold values from -120 to 120, as said below
- query_k: bfloat16 [64, 256, 1024], P('blk', None, 'head'), may hold values from -6 to 6
- query_v: bfloat16 [64, 256, 1024], P('blk', None, 'head'), may hold values from -6 to 6
- out_weight: bfloat16 [4096, 4096], P('head', 'blk'), may hold values from -0.09375 to 0.09375
- anchor_index: int32 [1], replicated, may hold values from 0 to 63
- owner_index: int32 [1], replicated, may hold values from 0 to 63
- counts: int32 [64], replicated, may hold values from 256 to 1024, as said below
Outputs:
- ctx_out: bfloat16 [65536, 4096], P('blk', 'head')
- answer: bfloat16 [256, 4096], P(None, 'blk')
The draws below stay inside these ranges and needn't reach their ends.
Inputs may be any that keep to these rules, and one draw needn't show every extreme that they name: `ctx_q`: row 5 mod 64 of a block or query slab may be a large multiple of a key row of the same head nearby. `query_q`: row 5 mod 64 of a slab may be a large multiple of a key row of the same head nearby. `counts`: some block has exactly 1024 valid tokens.
All inputs are finite; a program needn't handle non-finite values.
Results may differ from the reference program's by a relative error of at most 0.0056.
Values may be sent and summed in bfloat16 or wider, within the bound.
A program may use at most 128 MiB of HBM per device.

```python
import jax
import jax.numpy as jnp
from jax import lax

D = 4096
HEADS = 32
KV_HEADS = 8
HEAD_DIM = 128
BLOCK = 1024
QT = 256
CTX = 65536
N_BLK = 64


def shaped_pair(key, lead):
    group = HEADS // KV_HEADS
    keys = jnp.clip(jax.random.normal(jax.random.fold_in(key, 11), lead + (KV_HEADS, HEAD_DIM), jnp.float32), -6.0, 6.0)
    queries = jnp.clip(jax.random.normal(jax.random.fold_in(key, 12), lead + (KV_HEADS, group, HEAD_DIM), jnp.float32), -6.0, 6.0)
    return (queries.reshape(lead + (HEADS * HEAD_DIM,)).astype(jnp.bfloat16), keys.reshape(lead + (KV_HEADS * HEAD_DIM,)).astype(jnp.bfloat16))


def draw_ctx_q(key, part):
    return shaped_pair(key, (CTX,))[0]


def draw_ctx_k(key, part):
    return shaped_pair(key, (CTX,))[1]


def draw_query_q(key, part):
    return shaped_pair(jax.random.fold_in(key, 21), (N_BLK, QT))[0]


def draw_query_k(key, part):
    return shaped_pair(jax.random.fold_in(key, 21), (N_BLK, QT))[1]


def draw_counts(key, part):
    values = jax.random.randint(jax.random.fold_in(key, 31), (N_BLK,), BLOCK // 4, BLOCK + 1)
    full_block = jax.random.randint(jax.random.fold_in(key, 32), (), 0, N_BLK)
    return values.at[full_block].set(BLOCK).astype(jnp.int32)


def shard_levels(own_key, extent, shards, smallest, largest):
    def one(dim, shards_of):
        heights = jax.random.uniform(jax.random.fold_in(jax.random.fold_in(own_key, 6), dim), (shards_of,), jnp.float32, smallest / len(shards), largest / len(shards))
        return jnp.repeat(jnp.exp(heights), extent[dim] // shards_of).reshape((-1,) + (1,) * (len(extent) - dim - 1))

    loudness = one(*shards[0])
    for cut in shards[1:]:
        loudness = loudness * one(*cut)
    return loudness


def bell_draw(key, shape, spread, bound, pieces=(), kind=jnp.bfloat16):
    factor_of = shard_levels(key, shape, pieces, -0.22, 0.18) if pieces else 1.0
    values = jax.random.normal(key, shape, jnp.float32) * spread * factor_of
    return jnp.minimum(jnp.maximum(values, -bound), bound).astype(kind)


def setup_inputs(seed: int = 0) -> dict:
    streams_of = jax.random.split(jax.random.key(seed), 11)
    ctx_q = draw_ctx_q(jax.random.fold_in(streams_of[10], 71), 0)
    ctx_k = draw_ctx_k(jax.random.fold_in(streams_of[10], 71), 0)
    ctx_v = bell_draw(streams_of[2], (CTX, KV_HEADS * HEAD_DIM), 1.0, 6.0, ((0, 64), (1, 4)))
    query_q = draw_query_q(jax.random.fold_in(streams_of[10], 71), 0)
    query_k = draw_query_k(jax.random.fold_in(streams_of[10], 71), 0)
    query_v = bell_draw(streams_of[5], (N_BLK, QT, KV_HEADS * HEAD_DIM), 1.0, 6.0, ((0, 64), (2, 4)))
    out_weight = bell_draw(streams_of[6], (HEADS * HEAD_DIM, D), (HEADS * HEAD_DIM) ** -0.5, 0.09375, ((0, 4), (1, 64)))
    anchor_index = jax.random.randint(streams_of[7], (1,), 0, N_BLK).astype(jnp.int32)
    owner_index = jax.random.randint(streams_of[8], (1,), 0, N_BLK).astype(jnp.int32)
    counts = draw_counts(jax.random.fold_in(streams_of[10], 71), 0)
    return dict(ctx_q=ctx_q, ctx_k=ctx_k, ctx_v=ctx_v, query_q=query_q, query_k=query_k, query_v=query_v, out_weight=out_weight, anchor_index=anchor_index, owner_index=owner_index, counts=counts)


def attend(queries, keys, values, mask):
    scale = HEAD_DIM ** -0.5
    qh = queries.transpose(1, 0, 2, 3)
    kh = keys.transpose(1, 0, 2)
    vh = values.transpose(1, 0, 2)

    def one_head(item):
        qa, ka, va = item
        scores = jnp.einsum('rgd,kd->grk', qa.astype(jnp.float32), ka.astype(jnp.float32)) * scale
        scores = jnp.where(mask[None], scores, -1e30)
        top = jnp.max(scores, axis=-1)
        weights = jnp.where(mask[None], jnp.exp(scores - top[..., None]), 0.0)
        total = jnp.sum(weights, axis=-1)
        rounded = weights.astype(jnp.bfloat16).astype(jnp.float32)
        summed = jnp.einsum('grk,kd->grd', rounded, va.astype(jnp.float32))
        return top, total, summed

    return lax.map(one_head, (qh, kh, vh))


def combine(first, second):
    ma, la, oa = first
    mb, lb, ob = second
    top = jnp.maximum(ma, mb)
    ea = jnp.exp(ma - top)
    eb = jnp.exp(mb - top)
    return top, la * ea + lb * eb, oa * ea[..., None] + ob * eb[..., None]


def reference(ctx_q, ctx_k, ctx_v, query_q, query_k, query_v, out_weight, anchor_index, owner_index, counts):
    group = HEADS // KV_HEADS
    qb = ctx_q.reshape(N_BLK, BLOCK, KV_HEADS, group, HEAD_DIM)
    kb = ctx_k.reshape(N_BLK, BLOCK, KV_HEADS, HEAD_DIM)
    vb = ctx_v.reshape(N_BLK, BLOCK, KV_HEADS, HEAD_DIM)
    anchor = anchor_index[0]
    owner = owner_index[0]
    anchor_count = counts[anchor]
    row_pos = jnp.arange(BLOCK, dtype=jnp.int32)[:, None]
    col = jnp.arange(2 * BLOCK, dtype=jnp.int32)[None, :]
    inner = col - BLOCK

    def phase_one(index):
        own_count = counts[index]
        keys = jnp.concatenate([kb[anchor], kb[index]], axis=0)
        values = jnp.concatenate([vb[anchor], vb[index]], axis=0)
        mask = jnp.where(col < BLOCK, (col < anchor_count) & (index != anchor),
                         (inner <= row_pos) & (inner < own_count))
        top, total, summed = attend(qb[index], keys, values, mask)
        normed = summed / total[..., None]
        out = normed.transpose(2, 0, 1, 3).reshape(BLOCK, HEADS * HEAD_DIM)
        return jnp.where(row_pos < own_count, out, 0.0).astype(jnp.bfloat16)

    ctx_out = lax.map(phase_one, jnp.arange(N_BLK, dtype=jnp.int32)).reshape(CTX, HEADS * HEAD_DIM)

    query = query_q[owner].reshape(QT, KV_HEADS, group, HEAD_DIM)
    own_keys = query_k[owner].reshape(QT, KV_HEADS, HEAD_DIM)
    own_values = query_v[owner].reshape(QT, KV_HEADS, HEAD_DIM)
    qpos = jnp.arange(QT, dtype=jnp.int32)[:, None]
    col2 = jnp.arange(BLOCK + QT, dtype=jnp.int32)[None, :]
    inner2 = col2 - BLOCK

    def phase_two(carry, index):
        keys = jnp.concatenate([kb[index], own_keys], axis=0)
        values = jnp.concatenate([vb[index], own_values], axis=0)
        mask = jnp.where(col2 < BLOCK, col2 < counts[index], (inner2 <= qpos) & (index == owner))
        part = attend(query, keys, values, mask)
        return combine(carry, part), None

    start = (jnp.full((KV_HEADS, group, QT), -1e30, jnp.float32),
             jnp.zeros((KV_HEADS, group, QT), jnp.float32),
             jnp.zeros((KV_HEADS, group, QT, HEAD_DIM), jnp.float32))
    (top, total, summed), _ = lax.scan(phase_two, start, jnp.arange(N_BLK, dtype=jnp.int32))
    attn = (summed / total[..., None]).transpose(2, 0, 1, 3).reshape(QT, HEADS * HEAD_DIM).astype(jnp.bfloat16)
    answer = jnp.dot(attn, out_weight, preferred_element_type=jnp.float32).astype(jnp.bfloat16)
    return ctx_out, answer
```

```python
import functools

import jax
import jax.numpy as jnp
from jax import lax
from jax.experimental import pallas as pl
from jax.experimental.pallas import tpu as pltpu
from jax.sharding import Mesh
from jax.sharding import PartitionSpec as P

HEADS = 32
KV_HEADS = 8
HEAD_DIM = 128
BLK = ("blk_0", "blk_1", "blk_2")
NX, NZ, NY = 4, 8, 4
ROWS = 1024
QT = 256
LOCAL_KV = 2
GROUP = 4
LOCAL_HEADS = LOCAL_KV * GROUP
NEG = -1e30
SCALE2 = HEAD_DIM**-0.5 * 1.4426950408889634
F32 = jnp.float32
BF16 = jnp.bfloat16
MESH_ID = pl.DeviceIdType.MESH
RB = 256


def where_am_i():
    return tuple(lax.axis_index(a) for a in ("blk_0", "blk_1", "blk_2", "head"))


def greet(with_y):
    x, z, c, y = where_am_i()
    barrier = pltpu.get_barrier_semaphore()
    targets = [{"blk_2": 1 - c}]
    targets += [{"blk_0": lax.rem(x + d, NX)} for d in range(1, NX)]
    targets += [{"blk_1": lax.rem(z + d, NZ)} for d in range(1, NZ)]
    if with_y:
        targets += [{"head": lax.rem(y + d, NY)} for d in range(1, NY)]
    for t in targets:
        pl.semaphore_signal(barrier, inc=1, device_id=t, device_id_type=MESH_ID)
    pl.semaphore_wait(barrier, len(targets))


class Sems:
    def __init__(self, send, recv):
        self.send, self.recv, self.used = send, recv, 0

    def copy(self, src, dst, target):
        i = self.used
        self.used += 1
        return pltpu.make_async_remote_copy(
            src_ref=src,
            dst_ref=dst,
            send_sem=self.send.at[i],
            recv_sem=self.recv.at[i],
            device_id=target,
            device_id_type=MESH_ID,
        )


def start(copies):
    for c in copies:
        c.start()
    return copies


def arrived(copies):
    for c in copies:
        c.wait_recv()


def zslice(z, wide):
    if wide:
        return (
            pl.ds(pl.multiple_of(16 * (z // 4), 16), 16),
            pl.ds(pl.multiple_of(256 * lax.rem(z, 4), 256), 256),
        )
    return pl.ds(pl.multiple_of(16 * z, 16), 16), pl.ds(0, 256)


class Spread:
    def __init__(self, sems, src, out, s0, c1, sx, c2, sz, source, wide):
        self.sems, self.src, self.out = sems, src, out
        self.s0, self.c1, self.sx, self.c2, self.sz = s0, c1, sx, c2, sz
        self.fx, self.fz, self.fc = source
        self.wide = wide
        self.half = s0.shape[1]
        self.part = sx.shape[1]
        self.x, self.z, self.c, _ = where_am_i()
        self.copies = []

    def rows_half(self, c):
        return pl.ds(pl.multiple_of(self.half * c, self.half), self.half)

    def rows_x(self, c, x):
        return pl.ds(pl.multiple_of(self.half * c + self.part * x, self.part), self.part)

    def go(self, copies):
        self.copies += copies
        self.now = start(copies)

    def step0(self):
        other = 1 - self.c
        self.go([self.sems.copy(self.src.at[self.rows_half(other)], self.s0.at[self.c], {"blk_2": other})])
        self.s0[self.c] = self.src[self.rows_half(self.c), :]

    def step1(self):
        arrived(self.now)
        self.c1[...] = self.s0[self.fc]
        out = []
        for d in range(1, NX):
            t = lax.rem(self.x + d, NX)
            out.append(self.sems.copy(self.c1.at[self.rows_x(0, t)], self.sx.at[self.x], {"blk_0": t}))
        self.go(out)
        self.sx[self.x] = self.c1[self.rows_x(0, self.x), :]

    def step2(self):
        arrived(self.now)
        self.c2[...] = self.sx[self.fx]
        out = []
        for d in range(1, NZ):
            t = lax.rem(self.z + d, NZ)
            out.append(self.sems.copy(self.c2.at[zslice(t, self.wide)], self.sz.at[self.z], {"blk_1": t}))
        self.go(out)
        self.sz[self.z] = self.c2[zslice(self.z, self.wide)]

    def own(self):
        rows, cols = zslice(self.z, self.wide)
        start_row = self.half * self.c + self.part * self.x + (16 * (self.z // 4) if self.wide else 16 * self.z)
        return pl.ds(pl.multiple_of(start_row, 16), 16), cols

    def step3(self):
        arrived(self.now)
        self.out[self.own()] = self.sz[self.fz]
        self.share_z()

    def share_z(self):
        self.go(
            [
                self.sems.copy(self.out.at[self.own()], self.out.at[self.own()], {"blk_1": lax.rem(self.z + d, NZ)})
                for d in range(1, NZ)
            ]
        )

    def step4(self):
        arrived(self.now)
        piece = self.out.at[self.rows_x(self.c, self.x)]
        self.go([self.sems.copy(piece, piece, {"blk_0": lax.rem(self.x + d, NX)}) for d in range(1, NX)])

    def step5(self):
        arrived(self.now)
        piece = self.out.at[self.rows_half(self.c)]
        self.go([self.sems.copy(piece, piece, {"blk_2": 1 - self.c})])

    def step6(self):
        arrived(self.now)

    def finish(self):
        for c in self.copies:
            c.wait_send()


def coords(i):
    return i // (2 * NZ), lax.rem(i // 2, NZ), lax.rem(i, 2)


def spread_kernel(anchor_ref, owner_ref, q_ref, k_ref, v_ref, qo_ref, ko_ref, vo_ref, *rest):
    bufs, (send, recv) = rest[:15], rest[15:]
    sems = Sems(send, recv)
    greet(False)
    owner, anchor = coords(owner_ref[0]), coords(anchor_ref[0])
    q = Spread(sems, q_ref, qo_ref, *bufs[0:5], owner, True)
    k = Spread(sems, k_ref, ko_ref, *bufs[5:10], anchor, False)
    v = Spread(sems, v_ref, vo_ref, *bufs[10:15], anchor, False)
    for step in range(7):
        for a in (q, k, v):
            getattr(a, f"step{step}")()
    for a in (q, k, v):
        a.finish()


def spread_scratch():
    q = [
        pltpu.VMEM((2, 128, 1024), BF16),
        pltpu.VMEM((128, 1024), BF16),
        pltpu.VMEM((NX, 32, 1024), BF16),
        pltpu.VMEM((32, 1024), BF16),
        pltpu.VMEM((NZ, 16, 256), BF16),
    ]
    kv = [
        pltpu.VMEM((2, 512, 256), BF16),
        pltpu.VMEM((512, 256), BF16),
        pltpu.VMEM((NX, 128, 256), BF16),
        pltpu.VMEM((128, 256), BF16),
        pltpu.VMEM((NZ, 16, 256), BF16),
    ]
    return q + kv + kv


def nt(a, b):
    return lax.dot_general(a, b, (((1,), (1,)), ((), ())), preferred_element_type=F32)


def nn(a, b):
    return lax.dot_general(a, b, (((1,), (0,)), ((), ())), preferred_element_type=F32)


def iota(shape, dim):
    return lax.broadcasted_iota(jnp.int32, shape, dim)


def one_lane(rows):
    return jnp.where(iota((rows, 128), 1) == 0, 1.0, 0.0).astype(BF16)


def widen(k_ref, v_ref, ka, va, count):
    rows = k_ref.shape[0]
    hidden = (iota((rows, 128), 1) == 0) & (iota((rows, 128), 0) >= count)
    mask = jnp.where(hidden, NEG, 0.0).astype(BF16)
    ones = jnp.ones((rows, 128), BF16)
    for h in range(LOCAL_KV):
        cols = slice(h * 128, h * 128 + 128)
        ka[h, :, 0:128] = k_ref[:, cols]
        ka[h, :, 128:256] = mask
        va[h, :, 0:128] = v_ref[:, cols]
        va[h, :, 128:256] = ones


def head_cols(kv, g):
    return pl.ds(pl.multiple_of((kv * GROUP + g) * 128, 128), 128)


def own_part(kv, rb, q_ref, ka, va, o_own, m_own):
    rows = pl.ds(rb * RB, RB)
    lo = rb * RB
    e = one_lane(RB)
    tri = iota((RB, RB), 0) >= iota((RB, RB), 1)
    for g in range(GROUP):
        hh = kv * GROUP + g
        qa = jnp.concatenate([q_ref[rows, head_cols(kv, g)], e], axis=1)
        s2 = jnp.where(tri, nt(qa, ka[kv, lo : lo + RB, :]), NEG)
        m = jnp.max(s2, axis=1, keepdims=True)
        if rb:
            s1 = nt(qa, ka[kv, 0:lo, :])
            m = jnp.maximum(m, jnp.max(s1, axis=1, keepdims=True))
        p2 = jnp.exp2((s2 - m) * SCALE2).astype(BF16)
        acc = nn(p2, va[kv, lo : lo + RB, :])
        if rb:
            p1 = jnp.exp2((s1 - m) * SCALE2).astype(BF16)
            acc += nn(p1, va[kv, 0:lo, :])
        o_own[hh, rows, :] = acc
        m_own[hh, rows, :] = jnp.broadcast_to(m, (RB, 128))


def anchor_part(kv, rb, q_ref, ka, va, o_own, m_own, out_ref, own_count):
    row0 = pl.multiple_of(rb * RB, RB)
    rows = pl.ds(row0, RB)
    e = one_lane(RB)
    seen = iota((RB, 128), 0) + row0 < own_count
    for g in range(GROUP):
        hh = kv * GROUP + g
        cols = head_cols(kv, g)
        qa = jnp.concatenate([q_ref[rows, cols], e], axis=1)
        s = nt(qa, ka[kv])
        mo = m_own[hh, rows, :]
        m = jnp.maximum(mo, jnp.max(s, axis=1, keepdims=True))
        p = jnp.exp2((s - m[:, 0:1]) * SCALE2).astype(BF16)
        acc = nn(p, va[kv])
        a = jnp.exp2((mo - m) * SCALE2)
        o = acc[:, 0:128] + a * o_own[hh, rows, 0:128]
        total = acc[:, 128:256] + a * o_own[hh, rows, 128:256]
        out_ref[rows, cols] = jnp.where(seen, o / total, 0.0).astype(BF16)


def query_part(kv, q_ref, ka, va, kqa, vqa, part, stat):
    e = one_lane(QT)
    tri = iota((QT, QT), 0) >= iota((QT, QT), 1)
    lane = iota((QT, 128), 1)
    for g in range(GROUP):
        hh = kv * GROUP + g
        cols = head_cols(kv, g)
        qa = jnp.concatenate([q_ref[:, cols], e], axis=1)
        s1 = nt(qa, ka[kv])
        s2 = jnp.where(tri, nt(qa, kqa[kv]), NEG)
        m = jnp.maximum(jnp.max(s1, axis=1, keepdims=True), jnp.max(s2, axis=1, keepdims=True))
        p1 = jnp.exp2((s1 - m) * SCALE2).astype(BF16)
        p2 = jnp.exp2((s2 - m) * SCALE2).astype(BF16)
        acc = nn(p1, va[kv]) + nn(p2, vqa[kv])
        total = acc[:, 128:256]
        part[:, cols] = (acc[:, 0:128] / total).astype(BF16)
        stat[...] = jnp.where(lane == hh, m * SCALE2 + jnp.log2(total), stat[...])


def attend_kernel(
    anchor_ref, owner_ref, counts_ref, cq, ck, cv, ak, av, q, qk, qv, out, part,
    ka, va, kaa, vaa, kqa, vqa, o_own, m_own, stat,
):
    x, z, c, y = where_am_i()
    me = (x * NZ + z) * 2 + c
    anchor, owner = anchor_ref[0], owner_ref[0]
    own_count = counts_ref[me]
    anchor_count = jnp.where(me == anchor, 0, counts_ref[anchor])
    widen(ck, cv, ka, va, own_count)
    widen(ak, av, kaa, vaa, anchor_count)
    widen(qk, qv, kqa, vqa, jnp.where(me == owner, QT, 0))
    stat[...] = jnp.zeros_like(stat)

    @pl.loop(0, LOCAL_KV)
    def _(kv):
        query_part(kv, q, ka, va, kqa, vqa, part, stat)

    part[:, 1024:1152] = pack_stat(stat[...])
    for rb in range(ROWS // RB):

        @pl.loop(0, LOCAL_KV)
        def _(kv):
            own_part(kv, rb, cq, ka, va, o_own, m_own)

    @pl.loop(0, LOCAL_KV * (ROWS // RB))
    def _(i):
        anchor_part(i // 4, lax.rem(i, 4), cq, kaa, vaa, o_own, m_own, out, own_count)


def pack_stat(lse):
    lse = jnp.where(iota(lse.shape, 1) < 8, lse, 0.0)
    hi = lse.astype(BF16).astype(F32)
    mid = (lse - hi).astype(BF16).astype(F32)
    low = (lse - hi - mid).astype(BF16).astype(F32)
    return (hi + pltpu.roll(mid, 8, 1) + pltpu.roll(low, 16, 1)).astype(BF16)


def unpack_stat(stat):
    s = stat.astype(F32)
    return s + pltpu.roll(s, 120, 1) + pltpu.roll(s, 112, 1)


def merge(parts, stats, heads):
    lses = [unpack_stat(s) for s in stats]
    top = functools.reduce(jnp.maximum, lses)
    ws = [jnp.exp2(v - top) for v in lses]
    total = functools.reduce(jnp.add, ws)
    ws = [w / total for w in ws]
    outs = []
    for h in range(heads):
        acc = 0.0
        for w, o in zip(ws, parts):
            acc += w[:, h : h + 1] * o(h).astype(F32)
        outs.append(acc)
    return outs, top + jnp.log2(total)


def heads_of(ref, rows):
    return lambda h: ref[rows, h * 128 : h * 128 + 128]


class Combine:
    def __init__(self, sems, part, r0, p1, r1, p2, s2, r2o, r2s, attn):
        self.sems, self.part = sems, part
        self.r0, self.p1, self.r1, self.p2, self.s2, self.r2o, self.r2s = r0, p1, r1, p2, s2, r2o, r2s
        self.attn = attn
        self.x, self.z, self.c, self.y = where_am_i()
        self.copies = []

    def go(self, copies):
        self.copies += copies
        self.now = start(copies)

    def step0(self):
        other = 1 - self.c
        rows = pl.ds(pl.multiple_of(128 * other, 128), 128)
        self.go([self.sems.copy(self.part.at[rows], self.r0, {"blk_2": other})])

    def step1(self):
        arrived(self.now)
        lo = pl.multiple_of(128 * self.c, 128)

        @pl.loop(0, 4)
        def _(i):
            mine = pl.ds(pl.multiple_of(lo + 32 * i, 32), 32)
            theirs = pl.ds(pl.multiple_of(32 * i, 32), 32)
            outs, lse = merge(
                [heads_of(self.part, mine), heads_of(self.r0, theirs)],
                [self.part[mine, 1024:1152], self.r0[theirs, 1024:1152]],
                LOCAL_HEADS,
            )
            for h, o in enumerate(outs):
                self.p1[theirs, h * 128 : h * 128 + 128] = o.astype(BF16)
            self.p1[theirs, 1024:1152] = pack_stat(lse)

        def rows(x):
            return pl.ds(pl.multiple_of(32 * x, 32), 32)

        out = []
        for d in range(1, NX):
            t = lax.rem(self.x + d, NX)
            out.append(self.sems.copy(self.p1.at[rows(t)], self.r1.at[self.x], {"blk_0": t}))
        self.go(out)
        self.r1[self.x] = self.p1[rows(self.x), :]

    def step2(self):
        arrived(self.now)
        outs, lse = merge(
            [heads_of(self.r1.at[i], slice(0, 32)) for i in range(NX)],
            [self.r1[i, :, 1024:1152] for i in range(NX)],
            LOCAL_HEADS,
        )
        for h, o in enumerate(outs):
            self.p2[:, h * 128 : h * 128 + 128] = o.astype(BF16)
        for g in range(4):
            self.s2[g] = pack_stat(pltpu.roll(lse, 128 - 2 * g, 1) if g else lse)
        out = []
        for d in range(1, NZ):
            t = lax.rem(self.z + d, NZ)
            rows, cols = zslice(t, True)
            out.append(self.sems.copy(self.p2.at[rows, cols], self.r2o.at[self.z], {"blk_1": t}))
            out.append(self.sems.copy(self.s2.at[lax.rem(t, 4), rows], self.r2s.at[self.z], {"blk_1": t}))
        self.go(out)
        rows, cols = zslice(self.z, True)
        self.r2o[self.z] = self.p2[rows, cols]
        self.r2s[self.z] = self.s2[lax.rem(self.z, 4), rows, :]


def combine_kernel(part, w, ans, r0, p1, r1, p2, s2, r2o, r2s, attn, ry, send, recv):
    sems = Sems(send, recv)
    greet(True)
    x, z, c, y = where_am_i()
    comb = Combine(sems, part, r0, p1, r1, p2, s2, r2o, r2s, attn)
    comb.step0()
    comb.step1()
    comb.step2()
    arrived(comb.now)
    outs, _ = merge(
        [heads_of(r2o.at[i], slice(0, 16)) for i in range(NZ)], [r2s[i] for i in range(NZ)], 2
    )
    share = Share(sems, attn)
    share.put(jnp.concatenate(outs, axis=1).astype(BF16))
    share.share_z()
    share.step4()
    share.step5()
    share.step6()
    project(attn, w, ry, y)
    last = [
        sems.copy(ry.at[y], ry.at[y], {"head": lax.rem(y + d, NY)}) for d in range(1, NY)
    ]
    start(last)
    arrived(last)
    answer(ry, ans)
    for cp in comb.copies + share.copies + last:
        cp.wait_send()


class Share(Spread):
    def __init__(self, sems, out):
        self.sems, self.out, self.wide = sems, out, True
        self.half, self.part = 128, 32
        self.x, self.z, self.c, _ = where_am_i()
        self.copies = []

    def put(self, value):
        self.out[self.own()] = value


def project(attn, w, ry, y):
    ry[y] = jnp.concatenate([nn(attn[0:128, :], w[...]), nn(attn[128:256, :], w[...])], axis=1)


def answer(ry, ans):
    total = ((ry[0] + ry[1]) + ry[2]) + ry[3]
    ans[0:128, :] = total[:, 0:64].astype(BF16)
    ans[128:256, :] = total[:, 64:128].astype(BF16)


VM = pl.BlockSpec(memory_space=pltpu.VMEM)
SM = pl.BlockSpec(memory_space=pltpu.SMEM)


def shape(*dims, dtype=BF16):
    return jax.ShapeDtypeStruct(dims, dtype)


def per_device(ctx_q, ctx_k, ctx_v, query_q, query_k, query_v, out_weight, anchor_index, owner_index, counts):
    q, ak, av = pl.pallas_call(
        spread_kernel,
        out_shape=(shape(QT, 1024), shape(ROWS, 256), shape(ROWS, 256)),
        in_specs=[SM, SM, VM, VM, VM],
        out_specs=(VM, VM, VM),
        scratch_shapes=spread_scratch() + [pltpu.SemaphoreType.DMA((66,)), pltpu.SemaphoreType.DMA((66,))],
        compiler_params=pltpu.CompilerParams(collective_id=0, has_side_effects=True),
        name="spread",
    )(anchor_index, owner_index, query_q[0], ctx_k, ctx_v)
    ctx_out, part = pl.pallas_call(
        attend_kernel,
        out_shape=(shape(ROWS, 1024), shape(QT, 1152)),
        in_specs=[SM, SM, SM] + [VM] * 8,
        out_specs=(VM, VM),
        scratch_shapes=[
            pltpu.VMEM((LOCAL_KV, ROWS, 256), BF16),
            pltpu.VMEM((LOCAL_KV, ROWS, 256), BF16),
            pltpu.VMEM((LOCAL_KV, ROWS, 256), BF16),
            pltpu.VMEM((LOCAL_KV, ROWS, 256), BF16),
            pltpu.VMEM((LOCAL_KV, QT, 256), BF16),
            pltpu.VMEM((LOCAL_KV, QT, 256), BF16),
            pltpu.VMEM((LOCAL_HEADS, ROWS, 256), F32),
            pltpu.VMEM((LOCAL_HEADS, ROWS, 128), F32),
            pltpu.VMEM((QT, 128), F32),
        ],
        compiler_params=pltpu.CompilerParams(),
        name="attend",
    )(anchor_index, owner_index, counts, ctx_q, ctx_k, ctx_v, ak, av, q, query_k[0], query_v[0])
    ans = pl.pallas_call(
        combine_kernel,
        out_shape=shape(QT, 64),
        in_specs=[VM, VM],
        out_specs=VM,
        scratch_shapes=[
            pltpu.VMEM((128, 1152), BF16),
            pltpu.VMEM((128, 1152), BF16),
            pltpu.VMEM((NX, 32, 1152), BF16),
            pltpu.VMEM((32, 1024), BF16),
            pltpu.VMEM((4, 32, 128), BF16),
            pltpu.VMEM((NZ, 16, 256), BF16),
            pltpu.VMEM((NZ, 16, 128), BF16),
            pltpu.VMEM((QT, 1024), BF16),
            pltpu.VMEM((NY, 128, 128), F32),
            pltpu.SemaphoreType.DMA((32,)),
            pltpu.SemaphoreType.DMA((32,)),
        ],
        compiler_params=pltpu.CompilerParams(collective_id=1, has_side_effects=True),
        name="combine",
    )(part, out_weight)
    return ctx_out, ans


def solution(mesh):
    torus = Mesh(
        mesh.devices.reshape(NX, NZ, 2, mesh.shape["head"]), ("blk_0", "blk_1", "blk_2", "head")
    )
    placed = (
        P(BLK, "head"),
        P(BLK, "head"),
        P(BLK, "head"),
        P(BLK, None, "head"),
        P(BLK, None, "head"),
        P(BLK, None, "head"),
        P("head", BLK),
        P(),
        P(),
        P(),
    )
    return jax.shard_map(
        per_device,
        mesh=torus,
        in_specs=placed,
        out_specs=(P(BLK, "head"), P(None, BLK)),
        check_vma=False,
    )
```

```python
import functools

import jax
import jax.numpy as jnp
from jax import lax
from jax.experimental import pallas as pl
from jax.experimental.pallas import tpu as pltpu
from jax.sharding import Mesh
from jax.sharding import PartitionSpec as P

HEADS = 32
KV_HEADS = 8
HEAD_DIM = 128
BLK = ("blk_0", "blk_1", "blk_2")
NX, NZ, NY = 4, 8, 4
SIZE = {"blk_0": NX, "blk_1": NZ}
ROWS = 1024
QT = 256
LOCAL_KV = 2
GROUP = 4
LOCAL_HEADS = LOCAL_KV * GROUP
NEG = -1e30
VMEM_LIMIT = 52 << 20
SCALE2 = HEAD_DIM**-0.5 * 1.4426950408889634
F32 = jnp.float32
BF16 = jnp.bfloat16
MESH_ID = pl.DeviceIdType.MESH
RB = 256


def where_am_i():
    return tuple(lax.axis_index(a) for a in ("blk_0", "blk_1", "blk_2", "head"))


def plane_peers():
    x, z, c, y = where_am_i()
    out = []
    for dc in range(2):
        for dx in range(NX):
            for dy in range(NY):
                if dc or dx or dy:
                    out.append((lax.rem(x + dx, NX), lax.rem(c + dc, 2), lax.rem(y + dy, NY)))
    return out


def greet():
    z = lax.axis_index("blk_1")
    barrier = pltpu.get_barrier_semaphore()
    targets = [{"blk_1": lax.rem(z + d, NZ)} for d in range(1, NZ)]
    targets += [{"blk_0": px, "blk_2": pc, "head": py} for px, pc, py in plane_peers()]
    for t in targets:
        pl.semaphore_signal(barrier, inc=1, device_id=t, device_id_type=MESH_ID)
    pl.semaphore_wait(barrier, len(targets))


class Sems:
    def __init__(self, send, recv):
        self.send, self.recv, self.used = send, recv, 0

    def copy(self, src, dst, target):
        i = self.used
        self.used += 1
        return pltpu.make_async_remote_copy(
            src_ref=src,
            dst_ref=dst,
            send_sem=self.send.at[i],
            recv_sem=self.recv.at[i],
            device_id=target,
            device_id_type=MESH_ID,
        )


def start(copies):
    for c in copies:
        c.start()
    return copies


def arrived(copies):
    for c in copies:
        c.wait_recv()


def zslice(z):
    return (
        pl.ds(pl.multiple_of(16 * (z // 4), 16), 16),
        pl.ds(pl.multiple_of(128 * lax.rem(z, 4), 128), 128),
    )


def rows_at(start, size):
    return pl.ds(pl.multiple_of(start, 16), size)


class Spread:
    def __init__(self, sems, src, out, s0, c1, sx, c2, sz, source, order, wide):
        self.sems, self.src, self.out = sems, src, out
        self.s0, self.c1, self.sx, self.c2, self.sz = s0, c1, sx, c2, sz
        self.source = source
        self.setup(order, wide, s0.shape[1])

    def setup(self, order, wide, half):
        self.order, self.wide, self.half = order, wide, half
        x, z, c, _ = where_am_i()
        self.c = c
        self.me = {"blk_0": x, "blk_1": z}
        self.first, self.second = order
        self.part = half // SIZE[self.first]
        self.copies = []

    def peers(self, axis):
        return [lax.rem(self.me[axis] + d, SIZE[axis]) for d in range(1, SIZE[axis])]

    def rows_half(self, c):
        return rows_at(self.half * c, self.half)

    def rows_part(self, c, i):
        return rows_at(self.half * c + self.part * i, self.part)

    def slice2(self, i):
        if self.wide:
            return zslice(i)
        return rows_at(16 * i, 16), pl.ds(0, 256)

    def go(self, copies):
        self.copies += copies
        self.now = start(copies)

    def step0(self):
        other = 1 - self.c
        self.go([self.sems.copy(self.src.at[self.rows_half(other)], self.s0.at[self.c], {"blk_2": other})])
        self.s0[self.c] = self.src[self.rows_half(self.c), :]

    def step1(self):
        arrived(self.now)
        self.c1[...] = self.s0[self.source["blk_2"]]
        i = self.me[self.first]
        self.go(
            [
                self.sems.copy(self.c1.at[self.rows_part(0, t)], self.sx.at[i], {self.first: t})
                for t in self.peers(self.first)
            ]
        )
        self.sx[i] = self.c1[self.rows_part(0, i), :]

    def step2(self):
        arrived(self.now)
        self.c2[...] = self.sx[self.source[self.first]]
        i = self.me[self.second]
        self.go(
            [
                self.sems.copy(self.c2.at[self.slice2(t)], self.sz.at[i], {self.second: t})
                for t in self.peers(self.second)
            ]
        )
        self.sz[i] = self.c2[self.slice2(i)]

    def own(self):
        i = self.me[self.second]
        base = self.half * self.c + self.part * self.me[self.first]
        if self.wide:
            return rows_at(base + 16 * (i // 4), 16), zslice(i)[1]
        return rows_at(base + 16 * i, 16), pl.ds(0, 256)

    def step3(self):
        arrived(self.now)
        self.out[self.own()] = self.sz[self.source[self.second]]
        self.share()

    def share(self):
        piece = self.out.at[self.own()]
        self.go([self.sems.copy(piece, piece, {self.second: t}) for t in self.peers(self.second)])

    def step4(self):
        arrived(self.now)
        piece = self.out.at[self.rows_part(self.c, self.me[self.first])]
        self.go([self.sems.copy(piece, piece, {self.first: t}) for t in self.peers(self.first)])

    def step5(self):
        arrived(self.now)
        piece = self.out.at[self.rows_half(self.c)]
        self.go([self.sems.copy(piece, piece, {"blk_2": 1 - self.c})])

    def step6(self):
        arrived(self.now)


def coords(i):
    return {"blk_0": i // (2 * NZ), "blk_1": lax.rem(i // 2, NZ), "blk_2": lax.rem(i, 2)}


def spread_scratch(rows, width, order, wide):
    half = rows // 2
    part = half // SIZE[order[0]]
    return [
        pltpu.VMEM((2, half, width), BF16),
        pltpu.VMEM((half, width), BF16),
        pltpu.VMEM((SIZE[order[0]], part, width), BF16),
        pltpu.VMEM((part, width), BF16),
        pltpu.VMEM((SIZE[order[1]], 16, 128 if wide else 256), BF16),
    ]


def nt(a, b):
    return lax.dot_general(a, b, (((1,), (1,)), ((), ())), preferred_element_type=F32)


def nn(a, b):
    return lax.dot_general(a, b, (((1,), (0,)), ((), ())), preferred_element_type=F32)


def iota(shape, dim):
    return lax.broadcasted_iota(jnp.int32, shape, dim)


def one_lane(rows):
    return jnp.where(iota((rows, 128), 1) == 0, 1.0, 0.0).astype(BF16)


def widen(k_ref, v_ref, ka, va, count):
    rows = k_ref.shape[0]
    hidden = (iota((rows, 128), 1) == 0) & (iota((rows, 128), 0) >= count)
    mask = jnp.where(hidden, NEG, 0.0).astype(BF16)
    ones = jnp.ones((rows, 128), BF16)
    for h in range(LOCAL_KV):
        cols = slice(h * 128, h * 128 + 128)
        ka[h, :, 0:128] = k_ref[:, cols]
        ka[h, :, 128:256] = mask
        va[h, :, 0:128] = v_ref[:, cols]
        va[h, :, 128:256] = ones


def head_cols(kv, g):
    return pl.ds(pl.multiple_of((kv * GROUP + g) * 128, 128), 128)


def own_part(kv, rb, q_ref, ka, va, o_own, m_own):
    rows = pl.ds(rb * RB, RB)
    lo = rb * RB
    e = one_lane(RB)
    tri = iota((RB, RB), 0) >= iota((RB, RB), 1)
    for g in range(GROUP):
        hh = kv * GROUP + g
        qa = jnp.concatenate([q_ref[rows, head_cols(kv, g)], e], axis=1)
        s2 = jnp.where(tri, nt(qa, ka[kv, lo : lo + RB, :]), NEG)
        m = jnp.max(s2, axis=1, keepdims=True)
        if rb:
            s1 = nt(qa, ka[kv, 0:lo, :])
            m = jnp.maximum(m, jnp.max(s1, axis=1, keepdims=True))
        p2 = jnp.exp2((s2 - m) * SCALE2).astype(BF16)
        acc = nn(p2, va[kv, lo : lo + RB, :])
        if rb:
            p1 = jnp.exp2((s1 - m) * SCALE2).astype(BF16)
            acc += nn(p1, va[kv, 0:lo, :])
        o_own[hh, rows, :] = acc
        m_own[hh, rows, :] = jnp.broadcast_to(m, (RB, 128))


def anchor_part(kv, rb, q_ref, ka, va, o_own, m_own, out_ref, own_count):
    row0 = pl.multiple_of(rb * RB, RB)
    rows = pl.ds(row0, RB)
    e = one_lane(RB)
    seen = iota((RB, 128), 0) + row0 < own_count
    for g in range(GROUP):
        hh = kv * GROUP + g
        cols = head_cols(kv, g)
        qa = jnp.concatenate([q_ref[rows, cols], e], axis=1)
        s = nt(qa, ka[kv])
        mo = m_own[hh, rows, :]
        m = jnp.maximum(mo, jnp.max(s, axis=1, keepdims=True))
        p = jnp.exp2((s - m[:, 0:1]) * SCALE2).astype(BF16)
        acc = nn(p, va[kv])
        a = jnp.exp2((mo - m) * SCALE2)
        o = acc[:, 0:128] + a * o_own[hh, rows, 0:128]
        total = acc[:, 128:256] + a * o_own[hh, rows, 128:256]
        out_ref[rows, cols] = jnp.where(seen, o / total, 0.0).astype(BF16)


def self_part(kv, q_ref, kqa, vqa, o_self, m_self):
    e = one_lane(QT)
    row = iota((QT, QT), 0)
    at = lax.rem(row // 16, 2) * 128 + (row // 32) * 16 + lax.rem(row, 16)
    tri = at >= iota((QT, QT), 1)
    for g in range(GROUP):
        hh = kv * GROUP + g
        qa = jnp.concatenate([q_ref[kv, :, g * 128 : g * 128 + 128], e], axis=1)
        s = jnp.where(tri, nt(qa, kqa[kv]), NEG)
        m = jnp.max(s, axis=1, keepdims=True)
        o_self[hh] = nn(jnp.exp2((s - m) * SCALE2).astype(BF16), vqa[kv])
        m_self[hh] = jnp.broadcast_to(m, (QT, 128))


def query_part(kv, q_ref, ka, va, o_self, m_self, is_owner, part, part32):
    e = one_lane(QT)
    lane = iota((QT, 128), 1)
    stat = jnp.zeros((QT, 128), F32)
    for g in range(GROUP):
        hh = kv * GROUP + g
        cols = slice(g * 128, g * 128 + 128)
        qa = jnp.concatenate([q_ref[kv, :, cols], e], axis=1)
        s = nt(qa, ka[kv])
        ms = jnp.where(is_owner, m_self[hh], NEG)
        m = jnp.maximum(ms, jnp.max(s, axis=1, keepdims=True))
        p = jnp.exp2((s - m[:, 0:1]) * SCALE2).astype(BF16)
        acc = nn(p, va[kv])
        a = jnp.exp2((ms - m) * SCALE2)
        total = acc[:, 128:256] + a * o_self[hh, :, 128:256]
        o = (acc[:, 0:128] + a * o_self[hh, :, 0:128]) / total
        part32[kv, :, cols] = o
        part[kv, :, cols] = o.astype(BF16)
        stat = jnp.where(lane == g, m * SCALE2 + jnp.log2(total), stat)
    part[kv, :, 512:640] = pack_stat(stat)


def pack_stat(lse):
    lse = jnp.where(iota(lse.shape, 1) < 8, lse, 0.0)
    hi = lse.astype(BF16).astype(F32)
    mid = (lse - hi).astype(BF16).astype(F32)
    low = (lse - hi - mid).astype(BF16).astype(F32)
    return (hi + pltpu.roll(mid, 8, 1) + pltpu.roll(low, 16, 1)).astype(BF16)


def unpack_stat(stat):
    s = stat.astype(F32)
    return s + pltpu.roll(s, 120, 1) + pltpu.roll(s, 112, 1)


def merge(parts, stats, heads):
    lses = [unpack_stat(s) for s in stats]
    top = functools.reduce(jnp.maximum, lses)
    ws = [jnp.exp2(v - top) for v in lses]
    total = functools.reduce(jnp.add, ws)
    ws = [w / total for w in ws]
    outs = []
    for h in range(heads):
        acc = 0.0
        for w, o in zip(ws, parts):
            acc += w[:, h : h + 1] * o(h).astype(F32)
        outs.append(acc)
    return outs, top + jnp.log2(total)


def heads_of(ref, rows):
    return lambda h: ref[rows, h * 128 : h * 128 + 128]


class Combine:
    def __init__(self, sems, part, part32, r0, p1, p1f, r1, p2, p2f, s2, r2o, r2s):
        self.sems, self.part, self.part32 = sems, part, part32
        self.r0, self.p1, self.p1f, self.r1 = r0, p1, p1f, r1
        self.p2, self.p2f, self.s2, self.r2o, self.r2s = p2, p2f, s2, r2o, r2s
        self.x, self.z, self.c, self.y = where_am_i()
        self.copies = []

    def go(self, copies):
        self.copies += copies
        self.now = start(copies)

    def step0(self):
        other = 1 - self.c
        self.go([self.sems.copy(self.part.at[rows_at(128 * other, 128)], self.r0, {"blk_2": other})])

    def step1(self):
        arrived(self.now)

        @pl.loop(0, 4)
        def _(i):
            mine = rows_at(128 * self.c + 32 * i, 32)
            theirs = rows_at(32 * i, 32)
            outs, lse = merge(
                [heads_of(self.part32, mine), heads_of(self.r0, theirs)],
                [self.part[mine, 512:640], self.r0[theirs, 512:640]],
                GROUP,
            )
            for h, o in enumerate(outs):
                self.p1[theirs, h * 128 : h * 128 + 128] = o.astype(BF16)
                self.p1f[theirs, h * 128 : h * 128 + 128] = o
            self.p1[theirs, 512:640] = pack_stat(lse)

        out = []
        for d in range(1, NX):
            t = lax.rem(self.x + d, NX)
            out.append(self.sems.copy(self.p1.at[rows_at(32 * t, 32)], self.r1.at[d - 1], {"blk_0": t}))
        self.go(out)

    def step2(self):
        arrived(self.now)
        mine = rows_at(32 * self.x, 32)
        outs, lse = merge(
            [heads_of(self.p1f, mine)] + [heads_of(self.r1.at[i], slice(0, 32)) for i in range(NX - 1)],
            [self.p1[mine, 512:640]] + [self.r1[i, :, 512:640] for i in range(NX - 1)],
            GROUP,
        )
        for h, o in enumerate(outs):
            self.p2[:, h * 128 : h * 128 + 128] = o.astype(BF16)
            self.p2f[:, h * 128 : h * 128 + 128] = o
        for g in range(4):
            self.s2[g] = pack_stat(pltpu.roll(lse, 128 - g, 1) if g else lse)
        out = []
        for d in range(1, NZ):
            t = lax.rem(self.z + d, NZ)
            rows, cols = zslice(t)
            out.append(self.sems.copy(self.p2.at[rows, cols], self.r2o.at[d - 1], {"blk_1": t}))
            out.append(self.sems.copy(self.s2.at[lax.rem(t, 4), rows], self.r2s.at[d - 1], {"blk_1": t}))
        self.go(out)

    def step3(self):
        arrived(self.now)
        rows, cols = zslice(self.z)
        own = self.p2f[rows, cols]
        outs, _ = merge(
            [lambda h: own[:, h * 128 : h * 128 + 128]]
            + [heads_of(self.r2o.at[i], slice(0, 16)) for i in range(NZ - 1)],
            [self.s2[lax.rem(self.z, 4), rows, :]] + [self.r2s[i] for i in range(NZ - 1)],
            1,
        )
        return outs[0].astype(BF16)


class Share(Spread):
    def __init__(self, sems, out):
        self.sems, self.out = sems, out
        self.setup(("blk_0", "blk_1"), True, 128)

    def own(self):
        return zslice(self.me["blk_1"])


def project(attn, wall, sb):
    rows = jnp.concatenate([attn[0], attn[1]], axis=1)
    p = nt(rows, wall[...].reshape(512, 1024))
    for i in range(8):
        cols = slice(i * 64, i * 64 + 64)
        sb[i] = jnp.concatenate([p[0:16, cols], p[16:32, cols]], axis=1)


def answer(rf, ans):
    total = (((rf[0] + rf[1]) + rf[2]) + rf[3]).reshape(128, 128).T
    ans[:, 0:128] = total[0:64].astype(BF16)
    ans[:, 128:256] = total[64:128].astype(BF16)


XZ = ("blk_0", "blk_1")
ZX = ("blk_1", "blk_0")
N_LOCAL = 11
SCALARS = ("anchor", "owner", "counts")
N_REMOTE = 4 * 22 + 2 * (1 + 3 + 14 + 7) + 4 + 31


def scratch_list():
    kva = pltpu.VMEM((LOCAL_KV, ROWS, 256), BF16)
    kvq = pltpu.VMEM((LOCAL_KV, QT, 256), BF16)
    named = dict(
        cq=pltpu.VMEM((ROWS, 1024), BF16),
        ck=pltpu.VMEM((ROWS, 256), BF16),
        cv=pltpu.VMEM((ROWS, 256), BF16),
        q=pltpu.VMEM((2, QT, 512), BF16),
        qk=pltpu.VMEM((QT, 256), BF16),
        qv=pltpu.VMEM((QT, 256), BF16),
        wall=pltpu.VMEM((2, NX, 64, 1024), BF16),
        qo=pltpu.VMEM((2, QT, 512), BF16),
        ko=pltpu.VMEM((ROWS, 256), BF16),
        vo=pltpu.VMEM((ROWS, 256), BF16),
        ka=kva, va=kva, kaa=kva, vaa=kva, kqa=kvq, vqa=kvq,
        o_own=pltpu.VMEM((LOCAL_HEADS, ROWS, 256), F32),
        m_own=pltpu.VMEM((LOCAL_HEADS, ROWS, 128), F32),
        o_self=pltpu.VMEM((LOCAL_HEADS, QT, 256), F32),
        m_self=pltpu.VMEM((LOCAL_HEADS, QT, 128), F32),
        part=pltpu.VMEM((2, QT, 640), BF16),
        part32=pltpu.VMEM((2, QT, 512), F32),
        r0=pltpu.VMEM((2, 128, 640), BF16),
        p1=pltpu.VMEM((2, 128, 640), BF16),
        p1f=pltpu.VMEM((2, 128, 512), F32),
        r1=pltpu.VMEM((2, NX - 1, 32, 640), BF16),
        p2=pltpu.VMEM((2, 32, 512), BF16),
        p2f=pltpu.VMEM((2, 32, 512), F32),
        s2=pltpu.VMEM((2, 4, 32, 128), BF16),
        r2o=pltpu.VMEM((2, NZ - 1, 16, 128), BF16),
        r2s=pltpu.VMEM((2, NZ - 1, 16, 128), BF16),
        attn=pltpu.VMEM((2, 32, 512), BF16),
        sb=pltpu.VMEM((8, 16, 128), F32),
        rf=pltpu.VMEM((NY, 8, 16, 128), F32),
        anchor=pltpu.SMEM((1,), jnp.int32),
        owner=pltpu.SMEM((1,), jnp.int32),
        counts=pltpu.SMEM((64,), jnp.int32),
        local=pltpu.SemaphoreType.DMA((N_LOCAL,)),
        send=pltpu.SemaphoreType.DMA((N_REMOTE,)),
        recv=pltpu.SemaphoreType.DMA((N_REMOTE,)),
    )
    return named


def layer_kernel(*refs):
    scalars, inputs, (out_vmem, ans), rest = refs[:3], refs[3:10], refs[10:12], refs[12:]
    names = scratch_list()
    b = dict(zip(names, rest))
    bufs = rest[len(names) :]
    x, z, c, y = where_am_i()
    slot = c * NX + x
    local = b["local"]
    q_hbm = inputs[0]
    q_whole = []
    for kv in range(2):
        cols = pl.ds(512 * kv, 512)
        for i in range(8):
            for hi in range(2):
                pltpu.make_async_copy(
                    q_hbm.at[pl.ds(128 * hi + 16 * i, 16), cols],
                    b["q"].at[kv, pl.ds(32 * i + 16 * hi, 16)],
                    local.at[kv],
                ).start()
        q_whole.append(pltpu.make_async_copy(q_hbm.at[:, cols], b["q"].at[kv], local.at[kv]))
    targets = [b["ck"], b["cv"], b["wall"].at[c, x], b["qk"], b["qv"], b["cq"]]
    sources = [inputs[1], inputs[2], inputs[6], inputs[4], inputs[5], inputs[3]]
    loads = [
        pltpu.make_async_copy(src, dst, local.at[i + 2])
        for i, (src, dst) in enumerate(zip(sources, targets))
    ]
    start(loads)
    anchor_ref, owner_ref, counts_ref = (b[n] for n in SCALARS)
    ints = [
        pltpu.make_async_copy(src, b[n], local.at[i + 8]) for i, (src, n) in enumerate(zip(scalars, SCALARS))
    ]
    start(ints)
    greet()
    for l in ints:
        l.wait()
    me = (x * NZ + z) * 2 + c
    own_count = counts_ref[me]
    is_owner = me == owner_ref[0]
    anchor_count = jnp.where(me == anchor_ref[0], 0, counts_ref[anchor_ref[0]])
    sems = Sems(b["send"], b["recv"])
    owner, anchor = coords(owner_ref[0]), coords(anchor_ref[0])
    qs = [
        Spread(sems, b["q"].at[i], b["qo"].at[i], *bufs[5 * i : 5 * i + 5], owner, XZ, True)
        for i in range(2)
    ]
    k = Spread(sems, b["ck"], b["ko"], *bufs[10:15], anchor, ZX, False)
    v = Spread(sems, b["cv"], b["vo"], *bufs[15:20], anchor, XZ, False)
    combs = [
        Combine(sems, *[b[n].at[i] for n in COMBINE_BUFFERS]) for i in range(2)
    ]
    shares = [Share(sems, b["attn"].at[i]) for i in range(2)]
    wall = b["wall"]
    w_copies = []

    def own(rb, first=0):
        @pl.loop(first, first + 1 if rb == 3 else LOCAL_KV)
        def _(kv):
            own_part(kv, rb, b["cq"], b["ka"], b["va"], b["o_own"], b["m_own"])

    def ask(kv):
        query_part(
            kv, b["qo"], b["ka"], b["va"], b["o_self"], b["m_self"], is_owner, b["part"], b["part32"]
        )
        combs[kv].step0()

    def slots(lo, hi):
        for i in range(lo, hi):
            anchor_part(
                i % 2, i // 2, b["cq"], b["kaa"], b["vaa"], b["o_own"], b["m_own"], out_vmem, own_count
            )

    def w_along_x():
        loads[2].wait()
        for d in range(1, NX):
            w_copies.append(sems.copy(wall.at[c, x], wall.at[c, x], {"blk_0": lax.rem(x + d, NX)}))
        start(w_copies)

    def w_to_core():
        arrived(w_copies)
        w_copies.append(sems.copy(wall.at[c], wall.at[c], {"blk_2": 1 - c}))
        w_copies[-1].start()

    for i in range(2):
        q_whole[i].wait()
        qs[i].step0()
    loads[0].wait()
    k.step0()
    loads[1].wait()
    v.step0()
    widen(b["ck"], b["cv"], b["ka"], b["va"], own_count)
    qs[0].step1()
    qs[1].step1()
    k.step1()
    v.step1()
    for l in loads[3:]:
        l.wait()
    widen(b["qk"], b["qv"], b["kqa"], b["vqa"], QT)
    own(0)

    @pl.loop(0, LOCAL_KV)
    def _(kv):
        self_part(kv, b["q"], b["kqa"], b["vqa"], b["o_self"], b["m_self"])

    qs[0].step2()
    qs[1].step2()
    own(1)
    own(2)
    qs[0].step3()
    qs[1].step3()
    own(3, 0)
    k.step2()
    v.step2()
    own(3, 1)
    qs[0].step4()
    qs[1].step4()
    k.step3()
    v.step3()
    qs[0].step5()
    qs[1].step5()
    k.step4()
    qs[0].step6()
    v.step4()
    ask(0)
    qs[1].step6()
    ask(1)
    combs[0].step1()
    combs[1].step1()
    v.step5()
    k.step5()
    v.step6()
    k.step6()
    widen(b["ko"], b["vo"], b["kaa"], b["vaa"], anchor_count)
    slots(0, 2)
    combs[0].step2()
    combs[1].step2()
    w_along_x()
    slots(2, 4)
    for cb, sh in zip(combs, shares):
        sh.out[sh.own()] = cb.step3()
        sh.share()
    w_to_core()
    slots(4, 6)
    shares[0].step6()
    shares[1].step6()
    arrived(w_copies[3:])
    project(b["attn"], wall, b["sb"])
    last = []
    for px, pc, py in plane_peers():
        to = {"blk_0": px, "blk_2": pc, "head": py}
        last.append(sems.copy(b["sb"].at[pc * NX + px], b["rf"].at[y, slot], to))
    start(last)
    b["rf"][y, slot] = b["sb"][slot]
    slots(6, 8)
    arrived(last)
    answer(b["rf"], ans)
    groups = [o.copies for o in (*qs, k, v, *combs, *shares)] + [w_copies, last]
    for group in groups:
        for cp in group:
            cp.wait_send()


COMBINE_BUFFERS = ("part", "part32", "r0", "p1", "p1f", "r1", "p2", "p2f", "s2", "r2o", "r2s")
VM = pl.BlockSpec(memory_space=pltpu.VMEM)
SM = pl.BlockSpec(memory_space=pltpu.SMEM)
HB = pl.BlockSpec(memory_space=pl.ANY)


def shape(*dims, dtype=BF16):
    return jax.ShapeDtypeStruct(dims, dtype)


def per_device(ctx_q, ctx_k, ctx_v, query_q, query_k, query_v, out_weight, anchor_index, owner_index, counts):
    spreads = (
        spread_scratch(QT, 512, XZ, True) * 2
        + spread_scratch(ROWS, 256, ZX, False)
        + spread_scratch(ROWS, 256, XZ, False)
    )
    ctx_out, ans = pl.pallas_call(
        layer_kernel,
        out_shape=(pltpu.VMEM((ROWS, 1024), BF16), pltpu.VMEM((64, QT), BF16)),
        in_specs=[HB] * 10,
        out_specs=(VM, VM),
        scratch_shapes=list(scratch_list().values()) + spreads,
        compiler_params=pltpu.CompilerParams(collective_id=0, has_side_effects=True, vmem_limit_bytes=VMEM_LIMIT),
        name="layer",
    )(
        anchor_index, owner_index, counts, query_q[0], ctx_k, ctx_v, ctx_q, query_k[0], query_v[0], out_weight.T
    )
    return ctx_out, ans.T


def solution(mesh):
    torus = Mesh(
        mesh.devices.reshape(NX, NZ, 2, mesh.shape["head"]), ("blk_0", "blk_1", "blk_2", "head")
    )
    placed = (
        P(BLK, "head"),
        P(BLK, "head"),
        P(BLK, "head"),
        P(BLK, None, "head"),
        P(BLK, None, "head"),
        P(BLK, None, "head"),
        P("head", BLK),
        P(),
        P(),
        P(),
    )
    return jax.shard_map(
        per_device,
        mesh=torus,
        in_specs=placed,
        out_specs=(P(BLK, "head"), P(None, BLK)),
        check_vma=False,
    )
```

```python
import functools

import jax
import jax.numpy as jnp
from jax import lax
from jax.experimental import pallas as pl
from jax.experimental.pallas import tpu as pltpu
from jax.sharding import Mesh
from jax.sharding import PartitionSpec as P

HEADS = 32
KV_HEADS = 8
HEAD_DIM = 128
BLK = ("blk_0", "blk_1", "blk_2")
NX, NZ, NY = 4, 8, 4
SIZE = {"blk_0": NX, "blk_1": NZ}
ROWS = 1024
QT = 256
LOCAL_KV = 2
GROUP = 4
LOCAL_HEADS = LOCAL_KV * GROUP
NEG = -1e30
VMEM_LIMIT = 52 << 20
SCALE2 = HEAD_DIM**-0.5 * 1.4426950408889634
F32 = jnp.float32
BF16 = jnp.bfloat16
MESH_ID = pl.DeviceIdType.MESH
RB = 256


def where_am_i():
    return tuple(lax.axis_index(a) for a in ("blk_0", "blk_1", "blk_2", "head"))


def plane_peers():
    x, z, c, y = where_am_i()
    out = []
    for dc in range(2):
        for dx in range(NX):
            for dy in range(NY):
                if dc or dx or dy:
                    out.append((lax.rem(x + dx, NX), lax.rem(c + dc, 2), lax.rem(y + dy, NY)))
    return out


def greet():
    z = lax.axis_index("blk_1")
    barrier = pltpu.get_barrier_semaphore()
    targets = [{"blk_1": lax.rem(z + d, NZ)} for d in range(1, NZ)]
    targets += [{"blk_0": px, "blk_2": pc, "head": py} for px, pc, py in plane_peers()]
    for t in targets:
        pl.semaphore_signal(barrier, inc=1, device_id=t, device_id_type=MESH_ID)
    pl.semaphore_wait(barrier, len(targets))


class Sems:
    def __init__(self, send, recv):
        self.send, self.recv, self.used = send, recv, 0
        self.groups = []

    def go(self, copies, region):
        i = self.used
        self.used += 1

        def remote(src, dst, target):
            return pltpu.make_async_remote_copy(
                src_ref=src,
                dst_ref=dst,
                send_sem=self.send.at[i],
                recv_sem=self.recv.at[i],
                device_id=target,
                device_id_type=MESH_ID,
            )

        for src, dst, target in copies:
            remote(src, dst, target).start()
        whole = remote(region, region, copies[0][2])
        self.groups.append(whole)
        return whole

    def finish(self):
        for whole in self.groups:
            whole.wait_send()


def start(copies):
    for c in copies:
        c.start()


def zslice(z):
    return (
        pl.ds(pl.multiple_of(16 * (z // 4), 16), 16),
        pl.ds(pl.multiple_of(128 * lax.rem(z, 4), 128), 128),
    )


def rows_at(start, size):
    return pl.ds(pl.multiple_of(start, 16), size)


class Spread:
    def __init__(self, sems, src, out, s0, c1, sx, c2, sz, source, order, wide):
        self.sems, self.src, self.out = sems, src, out
        self.s0, self.c1, self.sx, self.c2, self.sz = s0, c1, sx, c2, sz
        self.source = source
        self.setup(order, wide, s0.shape[1])

    def setup(self, order, wide, half):
        self.order, self.wide, self.half = order, wide, half
        x, z, c, _ = where_am_i()
        self.c = c
        self.me = {"blk_0": x, "blk_1": z}
        self.first, self.second = order
        self.part = half // SIZE[self.first]

    def peers(self, axis):
        return [lax.rem(self.me[axis] + d, SIZE[axis]) for d in range(1, SIZE[axis])]

    def rows_half(self, c):
        return rows_at(self.half * c, self.half)

    def rows_part(self, c, i):
        return rows_at(self.half * c + self.part * i, self.part)

    def slice2(self, i):
        if self.wide:
            return zslice(i)
        return rows_at(16 * i, 16), pl.ds(0, 256)

    def some(self, slots, axis):
        return slots.at[0 : SIZE[axis] - 1]

    def step0(self):
        other = 1 - self.c
        copy = (self.src.at[self.rows_half(other)], self.s0.at[self.c], {"blk_2": other})
        self.now = self.sems.go([copy], self.s0.at[0])
        self.s0[self.c] = self.src[self.rows_half(self.c), :]

    def step1(self):
        self.now.wait_recv()
        self.c1[...] = self.s0[self.source["blk_2"]]
        i = self.me[self.first]
        self.now = self.sems.go(
            [
                (self.c1.at[self.rows_part(0, t)], self.sx.at[i], {self.first: t})
                for t in self.peers(self.first)
            ],
            self.some(self.sx, self.first),
        )
        self.sx[i] = self.c1[self.rows_part(0, i), :]

    def step2(self):
        self.now.wait_recv()
        self.c2[...] = self.sx[self.source[self.first]]
        i = self.me[self.second]
        self.now = self.sems.go(
            [
                (self.c2.at[self.slice2(t)], self.sz.at[i], {self.second: t})
                for t in self.peers(self.second)
            ],
            self.some(self.sz, self.second),
        )
        self.sz[i] = self.c2[self.slice2(i)]

    def own(self):
        i = self.me[self.second]
        base = self.half * self.c + self.part * self.me[self.first]
        if self.wide:
            return rows_at(base + 16 * (i // 4), 16), zslice(i)[1]
        return rows_at(base + 16 * i, 16), pl.ds(0, 256)

    def step3(self):
        self.now.wait_recv()
        self.out[self.own()] = self.sz[self.source[self.second]]
        self.share()

    sz = sx = None

    def share(self):
        piece = self.out.at[self.own()]
        self.now = self.sems.go(
            [(piece, piece, {self.second: t}) for t in self.peers(self.second)], self.some(self.sz, self.second)
        )

    def step4(self):
        self.now.wait_recv()
        piece = self.out.at[self.rows_part(self.c, self.me[self.first])]
        self.now = self.sems.go(
            [(piece, piece, {self.first: t}) for t in self.peers(self.first)], self.some(self.sx, self.first)
        )

    def step5(self):
        self.now.wait_recv()
        piece = self.out.at[self.rows_half(self.c)]
        self.now = self.sems.go([(piece, piece, {"blk_2": 1 - self.c})], self.s0.at[0])

    def step6(self):
        self.now.wait_recv()


def coords(i):
    return {"blk_0": i // (2 * NZ), "blk_1": lax.rem(i // 2, NZ), "blk_2": lax.rem(i, 2)}


def spread_scratch(rows, width, order, wide):
    half = rows // 2
    part = half // SIZE[order[0]]
    return [
        pltpu.VMEM((2, half, width), BF16),
        pltpu.VMEM((half, width), BF16),
        pltpu.VMEM((SIZE[order[0]], part, width), BF16),
        pltpu.VMEM((part, width), BF16),
        pltpu.VMEM((SIZE[order[1]], 16, 128 if wide else 256), BF16),
    ]


def nt(a, b):
    return lax.dot_general(a, b, (((1,), (1,)), ((), ())), preferred_element_type=F32)


def nn(a, b):
    return lax.dot_general(a, b, (((1,), (0,)), ((), ())), preferred_element_type=F32)


def iota(shape, dim):
    return lax.broadcasted_iota(jnp.int32, shape, dim)


def one_lane(rows):
    return jnp.where(iota((rows, 128), 1) == 0, 1.0, 0.0).astype(BF16)


def widen(k_ref, v_ref, ka, va, count):
    rows = k_ref.shape[0]
    hidden = (iota((rows, 128), 1) == 0) & (iota((rows, 128), 0) >= count)
    mask = jnp.where(hidden, NEG, 0.0).astype(BF16)
    ones = jnp.ones((rows, 128), BF16)
    for h in range(LOCAL_KV):
        cols = slice(h * 128, h * 128 + 128)
        ka[h, :, 0:128] = k_ref[:, cols]
        ka[h, :, 128:256] = mask
        va[h, :, 0:128] = v_ref[:, cols]
        va[h, :, 128:256] = ones


def head_cols(kv, g):
    return pl.ds(pl.multiple_of((kv * GROUP + g) * 128, 128), 128)


def own_part(kv, rb, q_ref, ka, va, o_own, m_own):
    rows = pl.ds(rb * RB, RB)
    lo = rb * RB
    e = one_lane(RB)
    tri = iota((RB, RB), 0) >= iota((RB, RB), 1)
    for g in range(GROUP):
        hh = kv * GROUP + g
        qa = jnp.concatenate([q_ref[rows, head_cols(kv, g)], e], axis=1)
        s2 = jnp.where(tri, nt(qa, ka[kv, lo : lo + RB, :]), NEG)
        m = jnp.max(s2, axis=1, keepdims=True)
        if rb:
            s1 = nt(qa, ka[kv, 0:lo, :])
            m = jnp.maximum(m, jnp.max(s1, axis=1, keepdims=True))
        p2 = jnp.exp2((s2 - m) * SCALE2).astype(BF16)
        acc = nn(p2, va[kv, lo : lo + RB, :])
        if rb:
            p1 = jnp.exp2((s1 - m) * SCALE2).astype(BF16)
            acc += nn(p1, va[kv, 0:lo, :])
        o_own[hh, rows, :] = acc
        m_own[hh, rows, :] = jnp.broadcast_to(m, (RB, 128))


def anchor_part(kv, rb, q_ref, ka, va, o_own, m_own, out_ref, own_count):
    row0 = pl.multiple_of(rb * RB, RB)
    rows = pl.ds(row0, RB)
    e = one_lane(RB)
    seen = iota((RB, 128), 0) + row0 < own_count
    for g in range(GROUP):
        hh = kv * GROUP + g
        cols = head_cols(kv, g)
        qa = jnp.concatenate([q_ref[rows, cols], e], axis=1)
        s = nt(qa, ka[kv])
        mo = m_own[hh, rows, :]
        m = jnp.maximum(mo, jnp.max(s, axis=1, keepdims=True))
        p = jnp.exp2((s - m[:, 0:1]) * SCALE2).astype(BF16)
        acc = nn(p, va[kv])
        a = jnp.exp2((mo - m) * SCALE2)
        o = acc[:, 0:128] + a * o_own[hh, rows, 0:128]
        total = acc[:, 128:256] + a * o_own[hh, rows, 128:256]
        out_ref[rows, cols] = jnp.where(seen, o / total, 0.0).astype(BF16)


def self_part(kv, q_ref, kqa, vqa, o_self, m_self):
    e = one_lane(QT)
    row = iota((QT, QT), 0)
    at = lax.rem(row // 16, 2) * 128 + (row // 32) * 16 + lax.rem(row, 16)
    tri = at >= iota((QT, QT), 1)
    for g in range(GROUP):
        hh = kv * GROUP + g
        qa = jnp.concatenate([q_ref[kv, :, g * 128 : g * 128 + 128], e], axis=1)
        s = jnp.where(tri, nt(qa, kqa[kv]), NEG)
        m = jnp.max(s, axis=1, keepdims=True)
        o_self[hh] = nn(jnp.exp2((s - m) * SCALE2).astype(BF16), vqa[kv])
        m_self[hh] = jnp.broadcast_to(m, (QT, 128))


def query_part(kv, q_ref, ka, va, o_self, m_self, is_owner, part, part32):
    e = one_lane(QT)
    lane = iota((QT, 128), 1)
    stat = jnp.zeros((QT, 128), F32)
    for g in range(GROUP):
        hh = kv * GROUP + g
        cols = slice(g * 128, g * 128 + 128)
        qa = jnp.concatenate([q_ref[kv, :, cols], e], axis=1)
        s = nt(qa, ka[kv])
        ms = jnp.where(is_owner, m_self[hh], NEG)
        m = jnp.maximum(ms, jnp.max(s, axis=1, keepdims=True))
        p = jnp.exp2((s - m[:, 0:1]) * SCALE2).astype(BF16)
        acc = nn(p, va[kv])
        a = jnp.exp2((ms - m) * SCALE2)
        total = acc[:, 128:256] + a * o_self[hh, :, 128:256]
        o = (acc[:, 0:128] + a * o_self[hh, :, 0:128]) / total
        part32[kv, :, cols] = o
        part[kv, :, cols] = o.astype(BF16)
        stat = jnp.where(lane == g, m * SCALE2 + jnp.log2(total), stat)
    part[kv, :, 512:640] = pack_stat(stat)


def pack_stat(lse):
    lse = jnp.where(iota(lse.shape, 1) < 8, lse, 0.0)
    hi = lse.astype(BF16).astype(F32)
    mid = (lse - hi).astype(BF16).astype(F32)
    low = (lse - hi - mid).astype(BF16).astype(F32)
    return (hi + pltpu.roll(mid, 8, 1) + pltpu.roll(low, 16, 1)).astype(BF16)


def unpack_stat(stat):
    s = stat.astype(F32)
    return s + pltpu.roll(s, 120, 1) + pltpu.roll(s, 112, 1)


def merge(parts, stats, heads):
    lses = [unpack_stat(s) for s in stats]
    top = functools.reduce(jnp.maximum, lses)
    ws = [jnp.exp2(v - top) for v in lses]
    total = functools.reduce(jnp.add, ws)
    ws = [w / total for w in ws]
    outs = []
    for h in range(heads):
        acc = 0.0
        for w, o in zip(ws, parts):
            acc += w[:, h : h + 1] * o(h).astype(F32)
        outs.append(acc)
    return outs, top + jnp.log2(total)


def heads_of(ref, rows):
    return lambda h: ref[rows, h * 128 : h * 128 + 128]


class Combine:
    def __init__(self, sems, part, part32, r0, p1, p1f, r1, p2, p2f, s2, r2o, r2s):
        self.sems, self.part, self.part32 = sems, part, part32
        self.r0, self.p1, self.p1f, self.r1 = r0, p1, p1f, r1
        self.p2, self.p2f, self.s2, self.r2o, self.r2s = p2, p2f, s2, r2o, r2s
        self.x, self.z, self.c, self.y = where_am_i()

    def step0(self):
        other = 1 - self.c
        copy = (self.part.at[rows_at(128 * other, 128)], self.r0, {"blk_2": other})
        self.now = self.sems.go([copy], self.r0)

    def step1(self):
        self.now.wait_recv()

        @pl.loop(0, 4)
        def _(i):
            mine = rows_at(128 * self.c + 32 * i, 32)
            theirs = rows_at(32 * i, 32)
            outs, lse = merge(
                [heads_of(self.part32, mine), heads_of(self.r0, theirs)],
                [self.part[mine, 512:640], self.r0[theirs, 512:640]],
                GROUP,
            )
            for h, o in enumerate(outs):
                self.p1[theirs, h * 128 : h * 128 + 128] = o.astype(BF16)
                self.p1f[theirs, h * 128 : h * 128 + 128] = o
            self.p1[theirs, 512:640] = pack_stat(lse)

        out = []
        for d in range(1, NX):
            t = lax.rem(self.x + d, NX)
            out.append((self.p1.at[rows_at(32 * t, 32)], self.r1.at[d - 1], {"blk_0": t}))
        self.now = self.sems.go(out, self.r1)

    def step2(self):
        self.now.wait_recv()
        mine = rows_at(32 * self.x, 32)
        outs, lse = merge(
            [heads_of(self.p1f, mine)] + [heads_of(self.r1.at[i], slice(0, 32)) for i in range(NX - 1)],
            [self.p1[mine, 512:640]] + [self.r1[i, :, 512:640] for i in range(NX - 1)],
            GROUP,
        )
        for h, o in enumerate(outs):
            self.p2[:, h * 128 : h * 128 + 128] = o.astype(BF16)
            self.p2f[:, h * 128 : h * 128 + 128] = o
        for g in range(4):
            self.s2[g] = pack_stat(pltpu.roll(lse, 128 - g, 1) if g else lse)
        stats, out = [], []
        for d in range(1, NZ):
            t = lax.rem(self.z + d, NZ)
            rows, cols = zslice(t)
            stats.append((self.s2.at[lax.rem(t, 4), rows], self.r2s.at[d - 1], {"blk_1": t}))
            out.append((self.p2.at[rows, cols], self.r2o.at[d - 1], {"blk_1": t}))
        self.now_stats = self.sems.go(stats, self.r2s)
        self.now = self.sems.go(out, self.r2o)

    def step3(self):
        self.now_stats.wait_recv()
        self.now.wait_recv()
        rows, cols = zslice(self.z)
        own = self.p2f[rows, cols]
        outs, _ = merge(
            [lambda h: own[:, h * 128 : h * 128 + 128]]
            + [heads_of(self.r2o.at[i], slice(0, 16)) for i in range(NZ - 1)],
            [self.s2[lax.rem(self.z, 4), rows, :]] + [self.r2s[i] for i in range(NZ - 1)],
            1,
        )
        return outs[0].astype(BF16)


class Share(Spread):
    def __init__(self, sems, out, slots):
        self.sems, self.out, self.slots = sems, out, slots
        self.setup(("blk_0", "blk_1"), True, 128)

    def own(self):
        return zslice(self.me["blk_1"])

    def some(self, slots, axis):
        return self.slots


def project(attn, wall, sb):
    rows = jnp.concatenate([attn[0], attn[1]], axis=1)
    p = nt(rows, wall[...].reshape(512, 1024))
    for i in range(8):
        cols = slice(i * 64, i * 64 + 64)
        sb[i] = jnp.concatenate([p[0:16, cols], p[16:32, cols]], axis=1)


def answer(rf, ans):
    total = (((rf[0:8] + rf[8:16]) + rf[16:24]) + rf[24:32]).reshape(128, 128).T
    ans[:, 0:128] = total[0:64].astype(BF16)
    ans[:, 128:256] = total[64:128].astype(BF16)


XZ = ("blk_0", "blk_1")
ZX = ("blk_1", "blk_0")
N_LOCAL = 11
SCALARS = ("anchor", "owner", "counts")
N_REMOTE = 4 * 6 + 2 * (4 + 1) + 3


def scratch_list():
    kva = pltpu.VMEM((LOCAL_KV, ROWS, 256), BF16)
    kvq = pltpu.VMEM((LOCAL_KV, QT, 256), BF16)
    named = dict(
        cq=pltpu.VMEM((ROWS, 1024), BF16),
        ck=pltpu.VMEM((ROWS, 256), BF16),
        cv=pltpu.VMEM((ROWS, 256), BF16),
        q=pltpu.VMEM((2, QT, 512), BF16),
        qk=pltpu.VMEM((QT, 256), BF16),
        qv=pltpu.VMEM((QT, 256), BF16),
        wall=pltpu.VMEM((2, NX, 64, 1024), BF16),
        qo=pltpu.VMEM((2, QT, 512), BF16),
        ko=pltpu.VMEM((ROWS, 256), BF16),
        vo=pltpu.VMEM((ROWS, 256), BF16),
        ka=kva, va=kva, kaa=kva, vaa=kva, kqa=kvq, vqa=kvq,
        o_own=pltpu.VMEM((LOCAL_HEADS, ROWS, 256), F32),
        m_own=pltpu.VMEM((LOCAL_HEADS, ROWS, 128), F32),
        o_self=pltpu.VMEM((LOCAL_HEADS, QT, 256), F32),
        m_self=pltpu.VMEM((LOCAL_HEADS, QT, 128), F32),
        part=pltpu.VMEM((2, QT, 640), BF16),
        part32=pltpu.VMEM((2, QT, 512), F32),
        r0=pltpu.VMEM((2, 128, 640), BF16),
        p1=pltpu.VMEM((2, 128, 640), BF16),
        p1f=pltpu.VMEM((2, 128, 512), F32),
        r1=pltpu.VMEM((2, NX - 1, 32, 640), BF16),
        p2=pltpu.VMEM((2, 32, 512), BF16),
        p2f=pltpu.VMEM((2, 32, 512), F32),
        s2=pltpu.VMEM((2, 4, 32, 128), BF16),
        r2o=pltpu.VMEM((2, NZ - 1, 16, 128), BF16),
        r2s=pltpu.VMEM((2, NZ - 1, 16, 128), BF16),
        attn=pltpu.VMEM((2, 32, 512), BF16),
        sb=pltpu.VMEM((8, 16, 128), F32),
        rf=pltpu.VMEM((NY * 8, 16, 128), F32),
        anchor=pltpu.SMEM((1,), jnp.int32),
        owner=pltpu.SMEM((1,), jnp.int32),
        counts=pltpu.SMEM((64,), jnp.int32),
        local=pltpu.SemaphoreType.DMA((N_LOCAL,)),
        send=pltpu.SemaphoreType.DMA((N_REMOTE,)),
        recv=pltpu.SemaphoreType.DMA((N_REMOTE,)),
    )
    return named


def layer_kernel(*refs):
    scalars, inputs, (out_vmem, ans), rest = refs[:3], refs[3:10], refs[10:12], refs[12:]
    names = scratch_list()
    b = dict(zip(names, rest))
    bufs = rest[len(names) :]
    x, z, c, y = where_am_i()
    slot = c * NX + x
    local = b["local"]
    q_hbm = inputs[0]
    q_whole = []
    for kv in range(2):
        cols = pl.ds(512 * kv, 512)
        for i in range(8):
            for hi in range(2):
                pltpu.make_async_copy(
                    q_hbm.at[pl.ds(128 * hi + 16 * i, 16), cols],
                    b["q"].at[kv, pl.ds(32 * i + 16 * hi, 16)],
                    local.at[kv],
                ).start()
        q_whole.append(pltpu.make_async_copy(q_hbm.at[:, cols], b["q"].at[kv], local.at[kv]))
    targets = [b["ck"], b["cv"], b["wall"].at[c, x], b["qk"], b["qv"], b["cq"]]
    sources = [inputs[1], inputs[2], inputs[6], inputs[4], inputs[5], inputs[3]]
    loads = [
        pltpu.make_async_copy(src, dst, local.at[i + 2])
        for i, (src, dst) in enumerate(zip(sources, targets))
    ]
    start(loads)
    anchor_ref, owner_ref, counts_ref = (b[n] for n in SCALARS)
    ints = [
        pltpu.make_async_copy(src, b[n], local.at[i + 8]) for i, (src, n) in enumerate(zip(scalars, SCALARS))
    ]
    start(ints)
    greet()
    for l in ints:
        l.wait()
    me = (x * NZ + z) * 2 + c
    own_count = counts_ref[me]
    is_owner = me == owner_ref[0]
    anchor_count = jnp.where(me == anchor_ref[0], 0, counts_ref[anchor_ref[0]])
    sems = Sems(b["send"], b["recv"])
    owner, anchor = coords(owner_ref[0]), coords(anchor_ref[0])
    qs = [
        Spread(sems, b["q"].at[i], b["qo"].at[i], *bufs[5 * i : 5 * i + 5], owner, XZ, True)
        for i in range(2)
    ]
    k = Spread(sems, b["ck"], b["ko"], *bufs[10:15], anchor, ZX, False)
    v = Spread(sems, b["cv"], b["vo"], *bufs[15:20], anchor, XZ, False)
    combs = [
        Combine(sems, *[b[n].at[i] for n in COMBINE_BUFFERS]) for i in range(2)
    ]
    shares = [Share(sems, b["attn"].at[i], b["r2o"].at[i]) for i in range(2)]
    wall = b["wall"]
    w_copies = []

    def own(rb, first=0):
        @pl.loop(first, first + 1 if rb == 3 else LOCAL_KV)
        def _(kv):
            own_part(kv, rb, b["cq"], b["ka"], b["va"], b["o_own"], b["m_own"])

    def ask(kv):
        query_part(
            kv, b["qo"], b["ka"], b["va"], b["o_self"], b["m_self"], is_owner, b["part"], b["part32"]
        )
        combs[kv].step0()

    def slots(lo, hi):
        for i in range(lo, hi):
            anchor_part(
                i % 2, i // 2, b["cq"], b["kaa"], b["vaa"], b["o_own"], b["m_own"], out_vmem, own_count
            )

    def w_along_x():
        loads[2].wait()
        mine = wall.at[c, x]
        to = [(mine, mine, {"blk_0": lax.rem(x + d, NX)}) for d in range(1, NX)]
        w_copies.append(sems.go(to, wall.at[0, 0:3]))

    def w_to_core():
        w_copies[0].wait_recv()
        w_copies.append(sems.go([(wall.at[c], wall.at[c], {"blk_2": 1 - c})], wall.at[0]))

    for i in range(2):
        q_whole[i].wait()
        qs[i].step0()
    loads[0].wait()
    k.step0()
    loads[1].wait()
    v.step0()
    widen(b["ck"], b["cv"], b["ka"], b["va"], own_count)
    qs[0].step1()
    qs[1].step1()
    k.step1()
    v.step1()
    for l in loads[3:]:
        l.wait()
    widen(b["qk"], b["qv"], b["kqa"], b["vqa"], QT)
    own(0)

    @pl.loop(0, LOCAL_KV)
    def _(kv):
        self_part(kv, b["q"], b["kqa"], b["vqa"], b["o_self"], b["m_self"])

    qs[0].step2()
    qs[1].step2()
    own(1)
    own(2)
    qs[0].step3()
    qs[1].step3()
    own(3, 0)
    k.step2()
    v.step2()
    own(3, 1)
    qs[0].step4()
    qs[1].step4()
    k.step3()
    v.step3()
    qs[0].step5()
    qs[1].step5()
    k.step4()
    qs[0].step6()
    v.step4()
    ask(0)
    qs[1].step6()
    ask(1)
    combs[0].step1()
    combs[1].step1()
    v.step5()
    k.step5()
    v.step6()
    k.step6()
    widen(b["ko"], b["vo"], b["kaa"], b["vaa"], anchor_count)
    slots(0, 2)
    combs[0].step2()
    combs[1].step2()
    w_along_x()
    slots(2, 4)
    for cb, sh in zip(combs, shares):
        sh.out[sh.own()] = cb.step3()
        sh.share()
    w_to_core()
    slots(4, 6)
    shares[0].step6()
    shares[1].step6()
    w_copies[1].wait_recv()
    project(b["attn"], wall, b["sb"])
    last = []
    for px, pc, py in plane_peers():
        to = {"blk_0": px, "blk_2": pc, "head": py}
        last.append((b["sb"].at[pc * NX + px], b["rf"].at[y * 8 + slot], to))
    final = sems.go(last, b["rf"].at[0:31])
    b["rf"][y * 8 + slot] = b["sb"][slot]
    slots(6, 8)
    final.wait_recv()
    answer(b["rf"], ans)
    sems.finish()


COMBINE_BUFFERS = ("part", "part32", "r0", "p1", "p1f", "r1", "p2", "p2f", "s2", "r2o", "r2s")
VM = pl.BlockSpec(memory_space=pltpu.VMEM)
SM = pl.BlockSpec(memory_space=pltpu.SMEM)
HB = pl.BlockSpec(memory_space=pl.ANY)


def shape(*dims, dtype=BF16):
    return jax.ShapeDtypeStruct(dims, dtype)


def per_device(ctx_q, ctx_k, ctx_v, query_q, query_k, query_v, out_weight, anchor_index, owner_index, counts):
    spreads = (
        spread_scratch(QT, 512, XZ, True) * 2
        + spread_scratch(ROWS, 256, ZX, False)
        + spread_scratch(ROWS, 256, XZ, False)
    )
    ctx_out, ans = pl.pallas_call(
        layer_kernel,
        out_shape=(pltpu.VMEM((ROWS, 1024), BF16), pltpu.VMEM((64, QT), BF16)),
        in_specs=[HB] * 10,
        out_specs=(VM, VM),
        scratch_shapes=list(scratch_list().values()) + spreads,
        compiler_params=pltpu.CompilerParams(collective_id=0, has_side_effects=True, vmem_limit_bytes=VMEM_LIMIT),
        name="layer",
    )(
        anchor_index, owner_index, counts, query_q[0], ctx_k, ctx_v, ctx_q, query_k[0], query_v[0], out_weight.T
    )
    return ctx_out, ans.T


def solution(mesh):
    torus = Mesh(
        mesh.devices.reshape(NX, NZ, 2, mesh.shape["head"]), ("blk_0", "blk_1", "blk_2", "head")
    )
    placed = (
        P(BLK, "head"),
        P(BLK, "head"),
        P(BLK, "head"),
        P(BLK, None, "head"),
        P(BLK, None, "head"),
        P(BLK, None, "head"),
        P("head", BLK),
        P(),
        P(),
        P(),
    )
    return jax.shard_map(
        per_device,
        mesh=torus,
        in_specs=placed,
        out_specs=(P(BLK, "head"), P(None, BLK)),
        check_vma=False,
    )
```

```python
import functools

import jax
import jax.numpy as jnp
from jax import lax
from jax.experimental import pallas as pl
from jax.experimental.pallas import tpu as pltpu
from jax.sharding import Mesh
from jax.sharding import PartitionSpec as P

HEADS = 32
KV_HEADS = 8
HEAD_DIM = 128
BLK = ("blk_0", "blk_1", "blk_2")
NX, NZ, NY = 4, 8, 4
SIZE = {"blk_0": NX, "blk_1": NZ}
ROWS = 1024
QT = 256
LOCAL_KV = 2
GROUP = 4
LOCAL_HEADS = LOCAL_KV * GROUP
NEG = -1e30
VMEM_LIMIT = 52 << 20
SCALE2 = HEAD_DIM**-0.5 * 1.4426950408889634
F32 = jnp.float32
BF16 = jnp.bfloat16
MESH_ID = pl.DeviceIdType.MESH
RB = 256


def where_am_i():
    return tuple(lax.axis_index(a) for a in ("blk_0", "blk_1", "blk_2", "head"))


def plane_peers():
    x, z, c, y = where_am_i()
    out = []
    for dc in range(2):
        for dx in range(NX):
            for dy in range(NY):
                if dc or dx or dy:
                    out.append((lax.rem(x + dx, NX), lax.rem(c + dc, 2), lax.rem(y + dy, NY)))
    return out


def greet():
    z = lax.axis_index("blk_1")
    barrier = pltpu.get_barrier_semaphore()
    targets = [{"blk_1": lax.rem(z + d, NZ)} for d in range(1, NZ)]
    targets += [{"blk_0": px, "blk_2": pc, "head": py} for px, pc, py in plane_peers()]
    for t in targets:
        pl.semaphore_signal(barrier, inc=1, device_id=t, device_id_type=MESH_ID)
    pl.semaphore_wait(barrier, len(targets))


class Sems:
    def __init__(self, send, recv):
        self.send, self.recv, self.used = send, recv, 0
        self.groups = []

    def go(self, copies, region):
        i = self.used
        self.used += 1

        def remote(src, dst, target):
            return pltpu.make_async_remote_copy(
                src_ref=src,
                dst_ref=dst,
                send_sem=self.send.at[i],
                recv_sem=self.recv.at[i],
                device_id=target,
                device_id_type=MESH_ID,
            )

        for src, dst, target in copies:
            remote(src, dst, target).start()
        whole = remote(region, region, copies[0][2])
        self.groups.append(whole)
        return whole

    def finish(self):
        for whole in self.groups:
            whole.wait_send()


def start(copies):
    for c in copies:
        c.start()


def zslice(z):
    return (
        pl.ds(pl.multiple_of(16 * (z // 4), 16), 16),
        pl.ds(pl.multiple_of(128 * lax.rem(z, 4), 128), 128),
    )


def rows_at(start, size):
    return pl.ds(pl.multiple_of(start, 16), size)


class Spread:
    def __init__(self, sems, src, out, s0, c1, sx, c2, sz, source, order, wide):
        self.sems, self.src, self.out = sems, src, out
        self.s0, self.c1, self.sx, self.c2, self.sz = s0, c1, sx, c2, sz
        self.source = source
        self.setup(order, wide, s0.shape[1])

    def setup(self, order, wide, half):
        self.order, self.wide, self.half = order, wide, half
        x, z, c, _ = where_am_i()
        self.c = c
        self.me = {"blk_0": x, "blk_1": z}
        self.first, self.second = order
        self.part = half // SIZE[self.first]

    def peers(self, axis):
        return [lax.rem(self.me[axis] + d, SIZE[axis]) for d in range(1, SIZE[axis])]

    def rows_half(self, c):
        return rows_at(self.half * c, self.half)

    def rows_part(self, c, i):
        return rows_at(self.half * c + self.part * i, self.part)

    def slice2(self, i):
        if self.wide:
            return zslice(i)
        return rows_at(16 * i, 16), pl.ds(0, 256)

    def some(self, slots, axis):
        return slots.at[0 : SIZE[axis] - 1]

    def step0(self):
        other = 1 - self.c
        copy = (self.src.at[self.rows_half(other)], self.s0.at[self.c], {"blk_2": other})
        self.now = self.sems.go([copy], self.s0.at[0])
        self.s0[self.c] = self.src[self.rows_half(self.c), :]

    def step1(self):
        self.now.wait_recv()
        self.c1[...] = self.s0[self.source["blk_2"]]
        i = self.me[self.first]
        self.now = self.sems.go(
            [
                (self.c1.at[self.rows_part(0, t)], self.sx.at[i], {self.first: t})
                for t in self.peers(self.first)
            ],
            self.some(self.sx, self.first),
        )
        self.sx[i] = self.c1[self.rows_part(0, i), :]

    def step2(self):
        self.now.wait_recv()
        self.c2[...] = self.sx[self.source[self.first]]
        i = self.me[self.second]
        self.now = self.sems.go(
            [
                (self.c2.at[self.slice2(t)], self.sz.at[i], {self.second: t})
                for t in self.peers(self.second)
            ],
            self.some(self.sz, self.second),
        )
        self.sz[i] = self.c2[self.slice2(i)]

    def own(self):
        i = self.me[self.second]
        base = self.half * self.c + self.part * self.me[self.first]
        if self.wide:
            return rows_at(base + 16 * (i // 4), 16), zslice(i)[1]
        return rows_at(base + 16 * i, 16), pl.ds(0, 256)

    def step3(self):
        self.now.wait_recv()
        self.out[self.own()] = self.sz[self.source[self.second]]
        self.share()

    sz = sx = None

    def share(self):
        piece = self.out.at[self.own()]
        self.now = self.sems.go(
            [(piece, piece, {self.second: t}) for t in self.peers(self.second)], self.some(self.sz, self.second)
        )

    def step4(self):
        self.now.wait_recv()
        piece = self.out.at[self.rows_part(self.c, self.me[self.first])]
        self.now = self.sems.go(
            [(piece, piece, {self.first: t}) for t in self.peers(self.first)], self.some(self.sx, self.first)
        )

    def step5(self):
        self.now.wait_recv()
        piece = self.out.at[self.rows_half(self.c)]
        self.now = self.sems.go([(piece, piece, {"blk_2": 1 - self.c})], self.s0.at[0])

    def step6(self):
        self.now.wait_recv()


def coords(i):
    return {"blk_0": i // (2 * NZ), "blk_1": lax.rem(i // 2, NZ), "blk_2": lax.rem(i, 2)}


def spread_scratch(rows, width, order, wide):
    half = rows // 2
    part = half // SIZE[order[0]]
    return [
        pltpu.VMEM((2, half, width), BF16),
        pltpu.VMEM((half, width), BF16),
        pltpu.VMEM((SIZE[order[0]], part, width), BF16),
        pltpu.VMEM((part, width), BF16),
        pltpu.VMEM((SIZE[order[1]], 16, 128 if wide else 256), BF16),
    ]


def nt(a, b):
    return lax.dot_general(a, b, (((1,), (1,)), ((), ())), preferred_element_type=F32)


def nn(a, b):
    return lax.dot_general(a, b, (((1,), (0,)), ((), ())), preferred_element_type=F32)


def iota(shape, dim):
    return lax.broadcasted_iota(jnp.int32, shape, dim)


def one_lane(rows):
    return jnp.where(iota((rows, 128), 1) == 0, 1.0, 0.0).astype(BF16)


def widen(k_ref, v_ref, ka, va, count):
    rows = k_ref.shape[0]
    hidden = (iota((rows, 128), 1) == 0) & (iota((rows, 128), 0) >= count)
    mask = jnp.where(hidden, NEG, 0.0).astype(BF16)
    ones = jnp.ones((rows, 128), BF16)
    for h in range(LOCAL_KV):
        cols = slice(h * 128, h * 128 + 128)
        ka[h, :, 0:128] = k_ref[:, cols]
        ka[h, :, 128:256] = mask
        va[h, :, 0:128] = v_ref[:, cols]
        va[h, :, 128:256] = ones


def head_cols(kv, g):
    return pl.ds(pl.multiple_of((kv * GROUP + g) * 128, 128), 128)


def own_part(kv, rb, q_ref, ka, va, o_own, m_own):
    rows = pl.ds(rb * RB, RB)
    lo = rb * RB
    e = one_lane(RB)
    tri = iota((RB, RB), 0) >= iota((RB, RB), 1)
    for g in range(GROUP):
        hh = kv * GROUP + g
        qa = jnp.concatenate([q_ref[rows, head_cols(kv, g)], e], axis=1)
        s2 = jnp.where(tri, nt(qa, ka[kv, lo : lo + RB, :]), NEG)
        m = jnp.max(s2, axis=1, keepdims=True)
        if rb:
            s1 = nt(qa, ka[kv, 0:lo, :])
            m = jnp.maximum(m, jnp.max(s1, axis=1, keepdims=True))
        p2 = jnp.exp2((s2 - m) * SCALE2).astype(BF16)
        acc = nn(p2, va[kv, lo : lo + RB, :])
        if rb:
            p1 = jnp.exp2((s1 - m) * SCALE2).astype(BF16)
            acc += nn(p1, va[kv, 0:lo, :])
        o_own[hh, rows, :] = acc
        m_own[hh, rows, :] = jnp.broadcast_to(m, (RB, 128))


def anchor_part(kv, rb, q_ref, ka, va, o_own, m_own, out_ref, own_count):
    row0 = pl.multiple_of(rb * RB, RB)
    rows = pl.ds(row0, RB)
    e = one_lane(RB)
    seen = iota((RB, 128), 0) + row0 < own_count
    for g in range(GROUP):
        hh = kv * GROUP + g
        cols = head_cols(kv, g)
        qa = jnp.concatenate([q_ref[rows, cols], e], axis=1)
        s = nt(qa, ka[kv])
        mo = m_own[hh, rows, :]
        m = jnp.maximum(mo, jnp.max(s, axis=1, keepdims=True))
        p = jnp.exp2((s - m[:, 0:1]) * SCALE2).astype(BF16)
        acc = nn(p, va[kv])
        a = jnp.exp2((mo - m) * SCALE2)
        o = acc[:, 0:128] + a * o_own[hh, rows, 0:128]
        total = acc[:, 128:256] + a * o_own[hh, rows, 128:256]
        out_ref[rows, cols] = jnp.where(seen, o / total, 0.0).astype(BF16)


def self_part(kv, q_ref, kqa, vqa, o_self, m_self):
    e = one_lane(QT)
    row = iota((QT, QT), 0)
    at = lax.rem(row // 16, 2) * 128 + (row // 32) * 16 + lax.rem(row, 16)
    tri = at >= iota((QT, QT), 1)
    for g in range(GROUP):
        hh = kv * GROUP + g
        qa = jnp.concatenate([q_ref[kv, :, g * 128 : g * 128 + 128], e], axis=1)
        s = jnp.where(tri, nt(qa, kqa[kv]), NEG)
        m = jnp.max(s, axis=1, keepdims=True)
        o_self[hh] = nn(jnp.exp2((s - m) * SCALE2).astype(BF16), vqa[kv])
        m_self[hh] = jnp.broadcast_to(m, (QT, 128))


def query_part(kv, q_ref, ka, va, o_self, m_self, is_owner, part, part32):
    e = one_lane(QT)
    lane = iota((QT, 128), 1)
    stat = jnp.zeros((QT, 128), F32)
    for g in range(GROUP):
        hh = kv * GROUP + g
        cols = slice(g * 128, g * 128 + 128)
        qa = jnp.concatenate([q_ref[kv, :, cols], e], axis=1)
        s = nt(qa, ka[kv])
        ms = jnp.where(is_owner, m_self[hh], NEG)
        m = jnp.maximum(ms, jnp.max(s, axis=1, keepdims=True))
        p = jnp.exp2((s - m[:, 0:1]) * SCALE2).astype(BF16)
        acc = nn(p, va[kv])
        a = jnp.exp2((ms - m) * SCALE2)
        total = acc[:, 128:256] + a * o_self[hh, :, 128:256]
        o = (acc[:, 0:128] + a * o_self[hh, :, 0:128]) / total
        part32[kv, :, cols] = o
        part[kv, :, cols] = o.astype(BF16)
        stat = jnp.where(lane == g, m * SCALE2 + jnp.log2(total), stat)
    part[kv, :, 512:640] = pack_stat(stat)


def pack_stat(lse):
    lse = jnp.where(iota(lse.shape, 1) < 8, lse, 0.0)
    hi = lse.astype(BF16).astype(F32)
    mid = (lse - hi).astype(BF16).astype(F32)
    low = (lse - hi - mid).astype(BF16).astype(F32)
    return (hi + pltpu.roll(mid, 8, 1) + pltpu.roll(low, 16, 1)).astype(BF16)


def unpack_stat(stat):
    s = stat.astype(F32)
    return s + pltpu.roll(s, 120, 1) + pltpu.roll(s, 112, 1)


def merge(parts, stats, heads):
    lses = [unpack_stat(s) for s in stats]
    top = functools.reduce(jnp.maximum, lses)
    ws = [jnp.exp2(v - top) for v in lses]
    total = functools.reduce(jnp.add, ws)
    ws = [w / total for w in ws]
    outs = []
    for h in range(heads):
        acc = 0.0
        for w, o in zip(ws, parts):
            acc += w[:, h : h + 1] * o(h).astype(F32)
        outs.append(acc)
    return outs, top + jnp.log2(total)


def heads_of(ref, rows):
    return lambda h: ref[rows, h * 128 : h * 128 + 128]


class Combine:
    def __init__(self, sems, part, part32, r0, p1, p1f, r1, p2, p2f, s2, r2o, r2s):
        self.sems, self.part, self.part32 = sems, part, part32
        self.r0, self.p1, self.p1f, self.r1 = r0, p1, p1f, r1
        self.p2, self.p2f, self.s2, self.r2o, self.r2s = p2, p2f, s2, r2o, r2s
        self.x, self.z, self.c, self.y = where_am_i()

    def step0(self):
        other = 1 - self.c
        copy = (self.part.at[rows_at(128 * other, 128)], self.r0, {"blk_2": other})
        self.now = self.sems.go([copy], self.r0)

    def step1(self):
        self.now.wait_recv()

        @pl.loop(0, 4)
        def _(i):
            mine = rows_at(128 * self.c + 32 * i, 32)
            theirs = rows_at(32 * i, 32)
            outs, lse = merge(
                [heads_of(self.part32, mine), heads_of(self.r0, theirs)],
                [self.part[mine, 512:640], self.r0[theirs, 512:640]],
                GROUP,
            )
            for h, o in enumerate(outs):
                self.p1[theirs, h * 128 : h * 128 + 128] = o.astype(BF16)
                self.p1f[theirs, h * 128 : h * 128 + 128] = o
            self.p1[theirs, 512:640] = pack_stat(lse)

        out = []
        for d in range(1, NX):
            t = lax.rem(self.x + d, NX)
            out.append((self.p1.at[rows_at(32 * t, 32)], self.r1.at[d - 1], {"blk_0": t}))
        self.now = self.sems.go(out, self.r1)

    def step2(self):
        self.now.wait_recv()
        mine = rows_at(32 * self.x, 32)
        outs, lse = merge(
            [heads_of(self.p1f, mine)] + [heads_of(self.r1.at[i], slice(0, 32)) for i in range(NX - 1)],
            [self.p1[mine, 512:640]] + [self.r1[i, :, 512:640] for i in range(NX - 1)],
            GROUP,
        )
        for h, o in enumerate(outs):
            self.p2[:, h * 128 : h * 128 + 128] = o.astype(BF16)
            self.p2f[:, h * 128 : h * 128 + 128] = o
        for g in range(4):
            self.s2[g] = pack_stat(pltpu.roll(lse, 128 - g, 1) if g else lse)
        stats, out = [], []
        for d in range(1, NZ):
            t = lax.rem(self.z + d, NZ)
            rows, cols = zslice(t)
            stats.append((self.s2.at[lax.rem(t, 4), rows], self.r2s.at[d - 1], {"blk_1": t}))
            out.append((self.p2.at[rows, cols], self.r2o.at[d - 1], {"blk_1": t}))
        self.now_stats = self.sems.go(stats, self.r2s)
        self.now = self.sems.go(out, self.r2o)

    def step3(self):
        self.now_stats.wait_recv()
        self.now.wait_recv()
        rows, cols = zslice(self.z)
        own = self.p2f[rows, cols]
        outs, _ = merge(
            [lambda h: own[:, h * 128 : h * 128 + 128]]
            + [heads_of(self.r2o.at[i], slice(0, 16)) for i in range(NZ - 1)],
            [self.s2[lax.rem(self.z, 4), rows, :]] + [self.r2s[i] for i in range(NZ - 1)],
            1,
        )
        return outs[0].astype(BF16)


class Share(Spread):
    def __init__(self, sems, out, slots):
        self.sems, self.out, self.slots = sems, out, slots
        self.setup(("blk_0", "blk_1"), True, 128)

    def own(self):
        return zslice(self.me["blk_1"])

    def some(self, slots, axis):
        return self.slots


def project(attn, wall, sb):
    rows = jnp.concatenate([attn[0], attn[1]], axis=1)
    p = nt(rows, wall[...].reshape(512, 1024))
    for i in range(8):
        cols = slice(i * 64, i * 64 + 64)
        sb[i] = jnp.concatenate([p[0:16, cols], p[16:32, cols]], axis=1).astype(BF16)


def answer(rf, ans):
    parts = [rf[8 * i : 8 * i + 8].astype(F32) for i in range(NY)]
    total = (((parts[0] + parts[1]) + parts[2]) + parts[3]).reshape(128, 128).T
    ans[:, 0:128] = total[0:64].astype(BF16)
    ans[:, 128:256] = total[64:128].astype(BF16)


XZ = ("blk_0", "blk_1")
ZX = ("blk_1", "blk_0")
N_LOCAL = 11
SCALARS = ("anchor", "owner", "counts")
N_REMOTE = 4 * 6 + 2 * (4 + 1) + 3


def scratch_list():
    kva = pltpu.VMEM((LOCAL_KV, ROWS, 256), BF16)
    kvq = pltpu.VMEM((LOCAL_KV, QT, 256), BF16)
    named = dict(
        cq=pltpu.VMEM((ROWS, 1024), BF16),
        ck=pltpu.VMEM((ROWS, 256), BF16),
        cv=pltpu.VMEM((ROWS, 256), BF16),
        q=pltpu.VMEM((2, QT, 512), BF16),
        qk=pltpu.VMEM((QT, 256), BF16),
        qv=pltpu.VMEM((QT, 256), BF16),
        wall=pltpu.VMEM((2, NX, 64, 1024), BF16),
        qo=pltpu.VMEM((2, QT, 512), BF16),
        ko=pltpu.VMEM((ROWS, 256), BF16),
        vo=pltpu.VMEM((ROWS, 256), BF16),
        ka=kva, va=kva, kaa=kva, vaa=kva, kqa=kvq, vqa=kvq,
        o_own=pltpu.VMEM((LOCAL_HEADS, ROWS, 256), F32),
        m_own=pltpu.VMEM((LOCAL_HEADS, ROWS, 128), F32),
        o_self=pltpu.VMEM((LOCAL_HEADS, QT, 256), F32),
        m_self=pltpu.VMEM((LOCAL_HEADS, QT, 128), F32),
        part=pltpu.VMEM((2, QT, 640), BF16),
        part32=pltpu.VMEM((2, QT, 512), F32),
        r0=pltpu.VMEM((2, 128, 640), BF16),
        p1=pltpu.VMEM((2, 128, 640), BF16),
        p1f=pltpu.VMEM((2, 128, 512), F32),
        r1=pltpu.VMEM((2, NX - 1, 32, 640), BF16),
        p2=pltpu.VMEM((2, 32, 512), BF16),
        p2f=pltpu.VMEM((2, 32, 512), F32),
        s2=pltpu.VMEM((2, 4, 32, 128), BF16),
        r2o=pltpu.VMEM((2, NZ - 1, 16, 128), BF16),
        r2s=pltpu.VMEM((2, NZ - 1, 16, 128), BF16),
        attn=pltpu.VMEM((2, 32, 512), BF16),
        sb=pltpu.VMEM((8, 16, 128), BF16),
        rf=pltpu.VMEM((NY * 8, 16, 128), BF16),
        anchor=pltpu.SMEM((1,), jnp.int32),
        owner=pltpu.SMEM((1,), jnp.int32),
        counts=pltpu.SMEM((64,), jnp.int32),
        local=pltpu.SemaphoreType.DMA((N_LOCAL,)),
        send=pltpu.SemaphoreType.DMA((N_REMOTE,)),
        recv=pltpu.SemaphoreType.DMA((N_REMOTE,)),
    )
    return named


def layer_kernel(*refs):
    scalars, inputs, (out_vmem, ans), rest = refs[:3], refs[3:10], refs[10:12], refs[12:]
    names = scratch_list()
    b = dict(zip(names, rest))
    bufs = rest[len(names) :]
    x, z, c, y = where_am_i()
    slot = c * NX + x
    local = b["local"]
    q_hbm = inputs[0]
    q_whole = []
    for kv in range(2):
        cols = pl.ds(512 * kv, 512)
        for i in range(8):
            for hi in range(2):
                pltpu.make_async_copy(
                    q_hbm.at[pl.ds(128 * hi + 16 * i, 16), cols],
                    b["q"].at[kv, pl.ds(32 * i + 16 * hi, 16)],
                    local.at[kv],
                ).start()
        q_whole.append(pltpu.make_async_copy(q_hbm.at[:, cols], b["q"].at[kv], local.at[kv]))
    targets = [b["ck"], b["cv"], b["wall"].at[c, x], b["qk"], b["qv"], b["cq"]]
    sources = [inputs[1], inputs[2], inputs[6], inputs[4], inputs[5], inputs[3]]
    loads = [
        pltpu.make_async_copy(src, dst, local.at[i + 2])
        for i, (src, dst) in enumerate(zip(sources, targets))
    ]
    start(loads)
    anchor_ref, owner_ref, counts_ref = (b[n] for n in SCALARS)
    ints = [
        pltpu.make_async_copy(src, b[n], local.at[i + 8]) for i, (src, n) in enumerate(zip(scalars, SCALARS))
    ]
    start(ints)
    greet()
    for l in ints:
        l.wait()
    me = (x * NZ + z) * 2 + c
    own_count = counts_ref[me]
    is_owner = me == owner_ref[0]
    anchor_count = jnp.where(me == anchor_ref[0], 0, counts_ref[anchor_ref[0]])
    sems = Sems(b["send"], b["recv"])
    owner, anchor = coords(owner_ref[0]), coords(anchor_ref[0])
    qs = [
        Spread(sems, b["q"].at[i], b["qo"].at[i], *bufs[5 * i : 5 * i + 5], owner, XZ, True)
        for i in range(2)
    ]
    k = Spread(sems, b["ck"], b["ko"], *bufs[10:15], anchor, ZX, False)
    v = Spread(sems, b["cv"], b["vo"], *bufs[15:20], anchor, XZ, False)
    combs = [
        Combine(sems, *[b[n].at[i] for n in COMBINE_BUFFERS]) for i in range(2)
    ]
    shares = [Share(sems, b["attn"].at[i], b["r2o"].at[i]) for i in range(2)]
    wall = b["wall"]
    w_copies = []

    def own(rb, first=0):
        @pl.loop(first, first + 1 if rb == 3 else LOCAL_KV)
        def _(kv):
            own_part(kv, rb, b["cq"], b["ka"], b["va"], b["o_own"], b["m_own"])

    def ask(kv):
        query_part(
            kv, b["qo"], b["ka"], b["va"], b["o_self"], b["m_self"], is_owner, b["part"], b["part32"]
        )
        combs[kv].step0()

    def slots(lo, hi):
        for i in range(lo, hi):
            anchor_part(
                i % 2, i // 2, b["cq"], b["kaa"], b["vaa"], b["o_own"], b["m_own"], out_vmem, own_count
            )

    def w_along_x():
        loads[2].wait()
        mine = wall.at[c, x]
        to = [(mine, mine, {"blk_0": lax.rem(x + d, NX)}) for d in range(1, NX)]
        w_copies.append(sems.go(to, wall.at[0, 0:3]))

    def w_to_core():
        w_copies[0].wait_recv()
        w_copies.append(sems.go([(wall.at[c], wall.at[c], {"blk_2": 1 - c})], wall.at[0]))

    for i in range(2):
        q_whole[i].wait()
        qs[i].step0()
    loads[0].wait()
    k.step0()
    loads[1].wait()
    v.step0()
    widen(b["ck"], b["cv"], b["ka"], b["va"], own_count)
    qs[0].step1()
    qs[1].step1()
    k.step1()
    for l in loads[3:]:
        l.wait()
    widen(b["qk"], b["qv"], b["kqa"], b["vqa"], QT)
    own(0)

    @pl.loop(0, LOCAL_KV)
    def _(kv):
        self_part(kv, b["q"], b["kqa"], b["vqa"], b["o_self"], b["m_self"])

    qs[0].step2()
    qs[1].step2()
    v.step1()
    own(1)
    own(2)
    qs[0].step3()
    qs[1].step3()
    own(3, 0)
    k.step2()
    v.step2()
    own(3, 1)
    qs[0].step4()
    qs[1].step4()
    k.step3()
    v.step3()
    qs[0].step5()
    qs[1].step5()
    k.step4()
    qs[0].step6()
    v.step4()
    ask(0)
    qs[1].step6()
    ask(1)
    combs[0].step1()
    combs[1].step1()
    v.step5()
    k.step5()
    v.step6()
    k.step6()
    widen(b["ko"], b["vo"], b["kaa"], b["vaa"], anchor_count)
    slots(0, 2)
    combs[0].step2()
    combs[1].step2()
    w_along_x()
    slots(2, 4)
    for cb, sh in zip(combs, shares):
        sh.out[sh.own()] = cb.step3()
        sh.share()
    w_to_core()
    slots(4, 6)
    shares[0].step6()
    shares[1].step6()
    w_copies[1].wait_recv()
    project(b["attn"], wall, b["sb"])
    last = []
    for px, pc, py in plane_peers():
        to = {"blk_0": px, "blk_2": pc, "head": py}
        last.append((b["sb"].at[pc * NX + px], b["rf"].at[y * 8 + slot], to))
    final = sems.go(last, b["rf"].at[0:31])
    b["rf"][y * 8 + slot] = b["sb"][slot]
    slots(6, 8)
    final.wait_recv()
    answer(b["rf"], ans)
    sems.finish()


COMBINE_BUFFERS = ("part", "part32", "r0", "p1", "p1f", "r1", "p2", "p2f", "s2", "r2o", "r2s")
VM = pl.BlockSpec(memory_space=pltpu.VMEM)
SM = pl.BlockSpec(memory_space=pltpu.SMEM)
HB = pl.BlockSpec(memory_space=pl.ANY)


def shape(*dims, dtype=BF16):
    return jax.ShapeDtypeStruct(dims, dtype)


def per_device(ctx_q, ctx_k, ctx_v, query_q, query_k, query_v, out_weight, anchor_index, owner_index, counts):
    spreads = (
        spread_scratch(QT, 512, XZ, True) * 2
        + spread_scratch(ROWS, 256, ZX, False)
        + spread_scratch(ROWS, 256, XZ, False)
    )
    ctx_out, ans = pl.pallas_call(
        layer_kernel,
        out_shape=(pltpu.VMEM((ROWS, 1024), BF16), pltpu.VMEM((64, QT), BF16)),
        in_specs=[HB] * 10,
        out_specs=(VM, VM),
        scratch_shapes=list(scratch_list().values()) + spreads,
        compiler_params=pltpu.CompilerParams(collective_id=0, has_side_effects=True, vmem_limit_bytes=VMEM_LIMIT),
        name="layer",
    )(
        anchor_index, owner_index, counts, query_q[0], ctx_k, ctx_v, ctx_q, query_k[0], query_v[0], out_weight.T
    )
    return ctx_out, ans.T


def solution(mesh):
    torus = Mesh(
        mesh.devices.reshape(NX, NZ, 2, mesh.shape["head"]), ("blk_0", "blk_1", "blk_2", "head")
    )
    placed = (
        P(BLK, "head"),
        P(BLK, "head"),
        P(BLK, "head"),
        P(BLK, None, "head"),
        P(BLK, None, "head"),
        P(BLK, None, "head"),
        P("head", BLK),
        P(),
        P(),
        P(),
    )
    return jax.shard_map(
        per_device,
        mesh=torus,
        in_specs=placed,
        out_specs=(P(BLK, "head"), P(None, BLK)),
        check_vma=False,
    )
```
